32 devices in a mesh: grp: 2 (over x), tp: 16 (over z, y, core).
Axes of the slice: x: 2, y: 2, z: 4, core: 2. Of those that a mesh axis runs over, the one named last changes fastest.
Arguments:
- hidden_in: float32 [8, 4608], P('grp'), parts along dimension 0, may hold values from -6 to 6
- prefill_cache: bfloat16 [16, 1, 2, 4, 16, 8, 256], P('tp', None, None, 'grp'), parts along dimension 3, may hold values from -6 to 6
- lengths: int32 [8], P('grp'), parts along dimension 0, may hold values from 1 to 127
- page_table: int32 [8, 16], P('grp'), parts along dimension 0, may hold values from 0 to 15, each once within a row
- qkv_weight: bfloat16 [1, 8192, 4608], P(None, 'tp'), may hold values from -0.09375 to 0.09375
- out_weight: bfloat16 [1, 4608, 4096], P(None, 'tp'), may hold values from -0.09375 to 0.09375
- gate_up_weight: bfloat16 [1, 2, 18432, 4608], P(None, None, 'tp'), may hold values from -0.09375 to 0.09375
- down_weight: bfloat16 [1, 18432, 4608], P(None, 'tp'), may hold values from -0.0625 to 0.0625
- norm_gains: float32 [1, 4, 4608], replicated, may hold values from 0.25 to 1.75
Outputs:
- hidden_out: float32 [8, 4608], P('grp', 'tp'), parts along dimension 0
- decode_cache: bfloat16 [16, 1, 2, 8, 8, 2048], P('tp', None, None, 'grp'), parts along dimension 3
The draws below stay inside these ranges and needn't reach their ends.
There are 2 independent parts, one for each index of `grp`. The reference program is written for one: setup_inputs(seed, part) draws one part's arguments, and reference() takes and returns one part's arrays. A program takes and returns all parts, laid end to end along the dimension named above; an argument that names none is the same for every part. Nothing has to cross between parts.
Inputs may be any that keep to these rules, and one draw needn't show every extreme that they name: Request r's new token takes position lengths[r]. Each row is a permutation of 0 to 15; page j of request r holds cache positions page_table[r, j] * 8 to page_table[r, j] * 8 + 7.
All inputs are finite; a program needn't handle non-finite values.
Results may differ from the reference program's by a relative error of at most 0.012.
The reference program's roundings to bfloat16 on the way (of `normed`, `projected`, `attended`, `mixed`, `ffn_in` and `active`) count: a program that leaves them out, or rounds other values in their place, can miss the bound.
Values may be sent and summed in bfloat16 or wider, within the bound.
A program may use at most 128 MiB of HBM per device.

```python
import jax
import jax.numpy as jnp
from jax import lax

D = 4608
HEADS = 32
KV_HEADS = 16
HEAD_DIM = 128
FF = 18432
PREFILL_TP = 8
LAYERS = 1
REQ_GROUP = 2
CTX_DEV = 8
BATCH = 4
CTX = 128
N_TP = 16


def touch_ends(entries, rng, smallest, high):
    spot = [jax.random.randint(jax.random.fold_in(rng, axis), (), 0, length) for axis, length in enumerate(entries.shape)]
    longest = entries.shape.index(max(entries.shape))
    next_to = spot[:longest] + [(spot[longest] + 1) % entries.shape[longest]] + spot[longest + 1:]
    return entries.at[tuple(spot)].set(smallest).at[tuple(next_to)].set(high)


def with_spikes(entries, own_key, source, target, blocks, factor):
    owner, partner = [(jnp.arange(entries.shape[axis_at]) // (entries.shape[axis_at] // blocks)).reshape([-1 if axis == axis_at else 1 for axis in range(entries.ndim)]) for axis_at in (source, target)]
    chosen = jax.random.permutation(own_key, blocks)[partner]
    strong = (owner == chosen) | (owner == (partner + blocks // 2) % blocks)
    return jnp.where(strong, factor * entries, entries)


def level_of(key, dims, pieces, smallest, largest):
    gain, own = 1.0, jax.random.fold_in(key, 6)
    for position, blocks in pieces:
        draws = jnp.exp(jax.random.uniform(jax.random.fold_in(own, position), (blocks,), jnp.float32, smallest / len(pieces), largest / len(pieces)))
        gain = gain * jnp.repeat(draws, dims[position] // blocks).reshape([-1 if axis == position else 1 for axis in range(len(dims))])
    return gain


def gaussian(stream_key, shape, width, most, cuts=(), kind=jnp.bfloat16):
    loudness = level_of(stream_key, shape, cuts, -0.22, 0.18) if cuts else 1.0
    drawn = jax.random.normal(stream_key, shape, jnp.float32) * width * loudness
    return jnp.minimum(jnp.maximum(drawn, -most), most).astype(kind)


def bell_draw_with(key, shape, deviation, reach, split, heavy, kind=jnp.bfloat16):
    array = deviation * jax.random.normal(key, shape, jnp.float32)
    if split:
        array = array * level_of(key, shape, split, -0.22, 0.18)
    return jnp.clip(with_spikes(array, jax.random.fold_in(key, 3), *heavy), -reach, reach).astype(kind)


def setup_inputs(seed: int = 0, part: int = 0) -> dict:
    key_list = jax.random.split(jax.random.key(seed), 10)
    own_keys = jax.random.split(jax.random.fold_in(key_list[9], part), 10)
    hidden_in = gaussian(own_keys[0], (BATCH, D), 1.0, 6.0, (), jnp.float32)
    prefill_cache = gaussian(own_keys[1], (N_TP, LAYERS, 2, REQ_GROUP, N_TP, CTX_DEV, KV_HEADS // PREFILL_TP * HEAD_DIM), 1.0, 6.0, ((0, 16),))
    lengths = touch_ends(jax.random.randint(own_keys[2], (BATCH,), 1, CTX), jax.random.fold_in(own_keys[2], 1), 1, CTX - 1).astype(jnp.int32)
    page_table = jax.vmap(lambda own: jax.random.permutation(own, N_TP))(jax.random.split(own_keys[3], BATCH)).reshape((BATCH, N_TP)).astype(jnp.int32)
    qkv_weight = gaussian(key_list[4], (LAYERS, (HEADS + 2 * KV_HEADS) * HEAD_DIM, D), D ** -0.5, 0.09375, ((1, 16),))
    out_weight = gaussian(key_list[5], (LAYERS, D, HEADS * HEAD_DIM), (HEADS * HEAD_DIM) ** -0.5, 0.09375, ((1, 16),))
    gate_up_weight = gaussian(key_list[6], (LAYERS, 2, FF, D), D ** -0.5, 0.09375, ((2, 16),))
    down_weight = bell_draw_with(key_list[7], (LAYERS, FF, D), FF ** -0.5, 0.0625, ((1, 16),), (1, 2, 16, 2.0))
    norm_gains = jnp.clip(1.0 + 0.15 * jax.random.normal(key_list[8], (LAYERS, 4, D), jnp.float32), 0.25, 1.75)
    return dict(hidden_in=hidden_in, prefill_cache=prefill_cache, lengths=lengths, page_table=page_table, qkv_weight=qkv_weight, out_weight=out_weight, gate_up_weight=gate_up_weight, down_weight=down_weight, norm_gains=norm_gains)


EPSILON = 1e-06
SOFTCAP = 50.0

def rms_scale(vector, gain_row):
    meansq = lax.optimization_barrier(jnp.mean(vector * vector, axis=-1, keepdims=True))
    return vector * lax.rsqrt(meansq + EPSILON) * (1.0 + gain_row)

def rotate(vector, positions):
    half_dim = vector.shape[-1] // 2
    exponent = jnp.arange(half_dim, dtype=jnp.float32) * (-2.0 / vector.shape[-1])
    frequency = jnp.power(jnp.float32(10000.0), exponent)
    angles = positions.astype(jnp.float32)[:, None, None] * frequency
    cosine = jnp.cos(angles)
    sine_term = jnp.sin(angles)
    front_half = vector[..., :half_dim]
    back_half = vector[..., half_dim:]
    return jnp.concatenate([front_half * cosine - back_half * sine_term, back_half * cosine + front_half * sine_term], axis=-1)

def capped(raw_scores):
    return SOFTCAP * jnp.tanh(raw_scores / SOFTCAP)

def round_back(vector):
    return lax.optimization_barrier(vector.astype(jnp.bfloat16)).astype(jnp.float32)

def reference(hidden_in, prefill_cache, lengths, page_table, qkv_weight, out_weight, gate_up_weight, down_weight, norm_gains):
    groups = N_TP // PREFILL_TP
    local_heads = KV_HEADS // PREFILL_TP
    head_share = HEADS // KV_HEADS
    score_scale = (D / HEADS) ** (-0.5)
    q_cols = HEADS * HEAD_DIM
    k_cols = KV_HEADS * HEAD_DIM
    blocks = prefill_cache.reshape(groups, PREFILL_TP, LAYERS, 2, REQ_GROUP, N_TP, CTX_DEV, local_heads, HEAD_DIM)
    by_request = blocks.transpose(2, 3, 0, 4, 5, 6, 1, 7, 8).reshape(LAYERS, 2, BATCH, N_TP, CTX_DEV, k_cols)
    page_ids = jnp.arange(N_TP, dtype=jnp.int32)
    onehot = (page_table[:, :, None] == page_ids[None, None, :]).astype(jnp.int32)
    inverse = lax.optimization_barrier(jnp.sum(onehot * page_ids[None, :, None], axis=1)).astype(jnp.int32)
    ordered = jnp.take_along_axis(by_request, inverse[None, None, :, :, None, None], axis=3)
    positions = page_ids[:, None] * CTX_DEV + jnp.arange(CTX_DEV, dtype=jnp.int32)[None, :]
    visible = positions[None, :, :] < lengths[:, None, None]
    fresh_slot = positions[None, :, :] == lengths[:, None, None]
    stream = hidden_in
    written = []
    for layer_index in range(LAYERS):
        normed = rms_scale(stream, norm_gains[layer_index, 0]).astype(jnp.bfloat16)
        projected = jnp.dot(normed, qkv_weight[layer_index].T, preferred_element_type=jnp.float32).astype(jnp.bfloat16)
        queries = rotate(projected[:, :q_cols].astype(jnp.float32).reshape(BATCH, HEADS, HEAD_DIM), lengths).astype(jnp.bfloat16)
        new_key = rotate(projected[:, q_cols:q_cols + k_cols].astype(jnp.float32).reshape(BATCH, KV_HEADS, HEAD_DIM), lengths).astype(jnp.bfloat16)
        new_value = projected[:, q_cols + k_cols:]
        key_layer = jnp.where(fresh_slot[:, :, :, None], new_key.reshape(BATCH, 1, 1, k_cols), ordered[layer_index, 0])
        value_layer = jnp.where(fresh_slot[:, :, :, None], new_value.reshape(BATCH, 1, 1, k_cols), ordered[layer_index, 1])
        written.append(jnp.stack([key_layer, value_layer], axis=0))
        shaped_q = queries.reshape(BATCH, KV_HEADS, head_share, HEAD_DIM).astype(jnp.float32)
        shaped_k = new_key.reshape(BATCH, KV_HEADS, 1, HEAD_DIM).astype(jnp.float32)
        shaped_v = new_value.reshape(BATCH, KV_HEADS, 1, HEAD_DIM).astype(jnp.float32)
        cached_keys = ordered[layer_index, 0].reshape(BATCH, N_TP, CTX_DEV, KV_HEADS, HEAD_DIM).astype(jnp.float32)
        cached_values = ordered[layer_index, 1].reshape(BATCH, N_TP, CTX_DEV, KV_HEADS, HEAD_DIM).astype(jnp.float32)
        raw_scores = jnp.einsum('bkmd,bjtkd->bkmjt', shaped_q, cached_keys) * score_scale
        weights = jnp.where(visible[:, None, None, :, :], jnp.exp(capped(raw_scores)), 0.0)
        own_weight = jnp.exp(capped(lax.optimization_barrier(jnp.sum(shaped_q * shaped_k, axis=-1)) * score_scale))
        denominator = lax.optimization_barrier(jnp.sum(weights, axis=(-2, -1))) + own_weight
        numerator = jnp.einsum('bkmjt,bjtkd->bkmd', round_back(weights), cached_values)
        numerator = numerator + round_back(own_weight)[..., None] * shaped_v
        attended = (numerator / denominator[..., None]).astype(jnp.bfloat16).reshape(BATCH, q_cols)
        mixed = jnp.dot(attended, out_weight[layer_index].T, preferred_element_type=jnp.float32).astype(jnp.bfloat16)
        stream = stream + rms_scale(mixed.astype(jnp.float32), norm_gains[layer_index, 1])
        ffn_in = rms_scale(stream, norm_gains[layer_index, 2]).astype(jnp.bfloat16)
        gate_proj = jnp.dot(ffn_in, gate_up_weight[layer_index, 0].T, preferred_element_type=jnp.float32)
        up_proj = jnp.dot(ffn_in, gate_up_weight[layer_index, 1].T, preferred_element_type=jnp.float32)
        active = (jax.nn.gelu(gate_proj, approximate=True) * up_proj).astype(jnp.bfloat16)
        branch = jnp.dot(active, down_weight[layer_index], preferred_element_type=jnp.float32)
        stream = stream + rms_scale(branch, norm_gains[layer_index, 3])
    decode_cache = jnp.stack(written, axis=0).transpose(3, 0, 1, 2, 4, 5)
    return (stream, decode_cache)
```

```python
import functools

import jax
import jax.numpy as jnp
from jax import lax
from jax.experimental import pallas as pl
from jax.experimental.pallas import tpu as pltpu
from jax.sharding import PartitionSpec as P

D = 4608
HEADS = 32
KV_HEADS = 16
HEAD_DIM = 128
PREFILL_TP = 8


EPSILON = 1e-06
SOFTCAP = 50.0


def rms_scale(vector, gain_row):
    meansq = jnp.mean(vector * vector, axis=-1, keepdims=True)
    return vector * lax.rsqrt(meansq + EPSILON) * (1.0 + gain_row)


def rotate(vector, positions):
    half_dim = vector.shape[-1] // 2
    exponent = jnp.arange(half_dim, dtype=jnp.float32) * (-2.0 / vector.shape[-1])
    frequency = jnp.power(jnp.float32(10000.0), exponent)
    angles = positions.astype(jnp.float32)[:, None, None] * frequency
    cosine = jnp.cos(angles)
    sine_term = jnp.sin(angles)
    front_half = vector[..., :half_dim]
    back_half = vector[..., half_dim:]
    return jnp.concatenate(
        [front_half * cosine - back_half * sine_term, back_half * cosine + front_half * sine_term],
        axis=-1,
    )


def capped(raw_scores):
    return SOFTCAP * jnp.tanh(raw_scores / SOFTCAP)


def round_back(vector):
    return lax.optimization_barrier(vector.astype(jnp.bfloat16)).astype(jnp.float32)


def pick_slot(vector, my_group, my_slot):
    inner = lax.dynamic_index_in_dim(vector, my_group, 0, False)
    return lax.dynamic_index_in_dim(inner, my_slot, 1, False)


def take_pages(page_block, page_order):
    return jnp.take(page_block, page_order, axis=2)


def project_rows(left, weight_rows):
    return jnp.einsum("bd,cd->bc", left, weight_rows, preferred_element_type=jnp.float32)


def on_device(
    hidden_in,
    prefill_cache,
    lengths,
    page_table,
    qkv_weight,
    out_weight,
    gate_up_weight,
    down_weight,
    norm_gains,
):
    devices = lax.axis_size("tp")
    my_index = lax.axis_index("tp")
    batch_rows = hidden_in.shape[0]
    groups = devices // PREFILL_TP
    per_group = batch_rows // groups
    local_heads = KV_HEADS // PREFILL_TP
    head_share = HEADS // KV_HEADS
    layer_count = prefill_cache.shape[1]
    page_width = prefill_cache.shape[5]
    score_scale = (D / HEADS) ** (-0.5)
    q_cols = HEADS * HEAD_DIM
    k_cols = KV_HEADS * HEAD_DIM
    my_group = my_index // PREFILL_TP
    my_slot = my_index % PREFILL_TP
    group_rows = lax.dynamic_slice_in_dim(page_table, my_group * per_group, per_group, 0)
    group_lengths = lax.dynamic_slice_in_dim(lengths, my_group * per_group, per_group, 0)
    local_cache = prefill_cache[0]
    page_ids = jnp.arange(devices, dtype=jnp.int32)
    onehot = (group_rows[:, :, None] == page_ids[None, None, :]).astype(jnp.int32)
    inverse = jnp.sum(onehot * page_ids[None, :, None], axis=1)
    arranged = jax.vmap(take_pages, in_axes=(2, 0), out_axes=2)(local_cache, inverse)
    relaid = lax.all_to_all(arranged, "tp", split_axis=3, concat_axis=3, tiled=True)
    relaid = relaid.reshape(
        layer_count, 2, per_group, groups, PREFILL_TP, page_width, local_heads, HEAD_DIM
    )
    decode_local = relaid.transpose(0, 1, 3, 2, 5, 4, 6, 7).reshape(
        layer_count, 2, batch_rows, page_width, k_cols
    )
    my_pos = my_index * page_width + jnp.arange(page_width, dtype=jnp.int32)
    fresh_slot = my_pos[None, :] == lengths[:, None]
    kept_cache = local_cache.reshape(
        layer_count, 2, per_group, devices, page_width, local_heads, HEAD_DIM
    )
    cache_pos = (
        group_rows[:, :, None] * page_width + jnp.arange(page_width, dtype=jnp.int32)[None, None, :]
    )
    kept_visible = cache_pos < group_lengths[:, None, None]
    stream = hidden_in
    normed = rms_scale(stream, norm_gains[0, 0]).astype(jnp.bfloat16)
    column_part = project_rows(normed, qkv_weight[0]).astype(jnp.bfloat16)
    projected = lax.all_gather(column_part, "tp", axis=1, tiled=True)
    queries = rotate(
        projected[:, :q_cols].astype(jnp.float32).reshape(batch_rows, HEADS, HEAD_DIM), lengths
    ).astype(jnp.bfloat16)
    new_key = rotate(
        projected[:, q_cols : q_cols + k_cols]
        .astype(jnp.float32)
        .reshape(batch_rows, KV_HEADS, HEAD_DIM),
        lengths,
    ).astype(jnp.bfloat16)
    new_value = projected[:, q_cols + k_cols :]
    key_layer = jnp.where(
        fresh_slot[:, :, None], new_key.reshape(batch_rows, 1, k_cols), decode_local[0, 0]
    )
    value_layer = jnp.where(
        fresh_slot[:, :, None], new_value.reshape(batch_rows, 1, k_cols), decode_local[0, 1]
    )
    written = [jnp.stack([key_layer, value_layer], axis=0)]
    flat_q = queries.reshape(batch_rows, KV_HEADS, head_share, HEAD_DIM)
    flat_k = new_key.reshape(batch_rows, KV_HEADS, 1, HEAD_DIM)
    flat_v = new_value.reshape(batch_rows, KV_HEADS, 1, HEAD_DIM)
    own_weight = jnp.exp(
        capped(
            jnp.sum(flat_q.astype(jnp.float32) * flat_k.astype(jnp.float32), axis=-1) * score_scale
        )
    )
    own_term = round_back(own_weight)[..., None] * flat_v.astype(jnp.float32)
    shaped_q = flat_q.reshape(groups, per_group, PREFILL_TP, local_heads, head_share, HEAD_DIM)
    shaped_own = own_weight.reshape(groups, per_group, PREFILL_TP, local_heads, head_share)
    shaped_term = own_term.reshape(groups, per_group, PREFILL_TP, local_heads, head_share, HEAD_DIM)
    my_queries = pick_slot(shaped_q, my_group, my_slot)
    cached_keys = kept_cache[0, 0]
    cached_values = kept_cache[0, 1]
    raw_scores = (
        jnp.einsum("ramd,rjcad->ramjc", my_queries, cached_keys, preferred_element_type=jnp.float32)
        * score_scale
    )
    weights = jnp.where(kept_visible[:, None, None, :, :], jnp.exp(capped(raw_scores)), 0.0)
    numerator = jnp.einsum(
        "ramjc,rjcad->ramd",
        weights.astype(jnp.bfloat16),
        cached_values,
        preferred_element_type=jnp.float32,
    )
    numerator = numerator + pick_slot(shaped_term, my_group, my_slot)
    denominator = jnp.sum(weights, axis=(-2, -1)) + pick_slot(shaped_own, my_group, my_slot)
    mine = (
        (numerator / denominator[..., None])
        .astype(jnp.bfloat16)
        .reshape(1, per_group, local_heads * head_share * HEAD_DIM)
    )
    gathered = lax.all_gather(mine, "tp", axis=0, tiled=True)
    attended = (
        gathered.reshape(groups, PREFILL_TP, per_group, local_heads * head_share * HEAD_DIM)
        .transpose(0, 2, 1, 3)
        .reshape(batch_rows, q_cols)
    )
    mixed_part = project_rows(attended, out_weight[0]).astype(jnp.bfloat16)
    mixed_out = lax.all_gather(mixed_part, "tp", axis=1, tiled=True)
    stream = stream + rms_scale(mixed_out.astype(jnp.float32), norm_gains[0, 1])
    ffn_in = rms_scale(stream, norm_gains[0, 2]).astype(jnp.bfloat16)
    gate_proj = project_rows(ffn_in, gate_up_weight[0, 0])
    up_proj = project_rows(ffn_in, gate_up_weight[0, 1])
    active = (jax.nn.gelu(gate_proj, approximate=True) * up_proj).astype(jnp.bfloat16)
    branch = jnp.dot(active, down_weight[0], preferred_element_type=jnp.float32)
    column_count = branch.shape[1] // devices
    summed = lax.psum(branch, "tp")
    stream = stream + rms_scale(summed, norm_gains[0, 3])
    result = lax.dynamic_slice_in_dim(stream, my_index * column_count, column_count, 1)
    decode_cache = jnp.stack(written, axis=0)[None]
    return (result, decode_cache)


MESH = pl.DeviceIdType.MESH
LANES = 128
NT = (((1,), (1,)), ((), ()))
LOG_BASE = 9.210340371976184
UNROLL = True
VMEM_LIMIT = 58 * 1024 * 1024


def dot_t(left, right):
    return lax.dot_general(left, right, NT, preferred_element_type=jnp.float32)


def normed_by(vector, meansq, gain):
    return vector * lax.rsqrt(meansq + EPSILON) * (1.0 + gain)


def meansq_of(vector):
    return jnp.mean(vector * vector, axis=-1, keepdims=True)


def column_of(scalars, count):
    row = lax.broadcasted_iota(jnp.int32, (count, 1), 0)
    column = jnp.zeros((count, 1), jnp.int32)
    for i in range(count):
        column = jnp.where(row == i, scalars[i], column)
    return column.astype(jnp.float32)


def pad_rows(rows, count):
    return jnp.concatenate(
        [rows, jnp.zeros((count - rows.shape[0], rows.shape[1]), rows.dtype)], axis=0
    )


def fused_kernel(
    dims,
    len_hbm,
    table_hbm,
    hid_hbm,
    gain_hbm,
    flat_hbm,
    wq_hbm,
    wo_hbm,
    wgu_hbm,
    wd_hbm,
    out_ref,
    dec_done,
    len_ref,
    hid,
    gain,
    table,
    flat,
    wq,
    wo,
    wgu,
    wd,
    proj,
    att,
    attended,
    mix,
    branch,
    arrive,
    sums,
    squares,
    turned_act,
    page_stage,
    dec,
    load_sem,
    send_sem,
    proj_sem,
    att_sem,
    mix_sem,
    tail_sem,
):
    T, B, R, RP = dims["T"], dims["B"], dims["R"], dims["RP"]
    share, local_heads, slots = dims["share"], dims["local_heads"], dims["S"]
    per_group, groups = dims["per_group"], dims["groups"]
    planes, plane_size = dims["planes"], dims["plane_size"]
    first_owner, owner_count = dims["first_owner"], dims["owner_count"]
    width = local_heads * HEAD_DIM
    cols = wq.shape[0]
    heads_here = cols // HEAD_DIM
    q_devs = HEADS * HEAD_DIM // cols
    k_devs = KV_HEADS * HEAD_DIM // cols
    page_width = dec.shape[2]
    model = wq.shape[1]
    ff = wd.shape[0]
    chunks = model // LANES
    score_scale = (D / HEADS) ** (-0.5)
    me = lax.axis_index("tp")
    my_group = me // PREFILL_TP
    my_slot = me % PREFILL_TP
    my_plane = me // plane_size
    my_seat = me % plane_size

    def load(index, src, dst):
        return pltpu.make_async_copy(src, dst, load_sem.at[index])

    small = [
        load(0, hid_hbm, hid.at[:, pl.ds(0, model)]),
        load(1, gain_hbm, gain.at[:, pl.ds(0, model)]),
        load(2, len_hbm, len_ref),
        load(3, table_hbm, table),
    ]
    cuts = dims["cuts"]
    wq_loads = [
        load(8 + i, wq_hbm.at[:, pl.ds(lo, hi - lo)], wq.at[:, pl.ds(lo, hi - lo)])
        for i, (lo, hi) in enumerate(cuts)
    ]
    flat_load = load(4, flat_hbm, flat)
    wo_load = load(5, wo_hbm, wo)
    wgu_load = load(6, wgu_hbm, wgu)
    wd_load = load(7, wd_hbm, wd)
    for piece in small + wq_loads + [flat_load]:
        piece.start()

    barrier = pltpu.get_barrier_semaphore()

    def greet(step, carry):
        peer = lax.rem(me + step, T)
        pl.semaphore_signal(barrier, inc=1, device_id={"tp": peer}, device_id_type=MESH)
        return carry

    lax.fori_loop(1, T, greet, 0)

    def dec_part(ref, index):
        group, slot = index // PREFILL_TP, index % PREFILL_TP
        lane = pl.multiple_of(slot * width, width)
        return ref.at[:, pl.ds(group * per_group, per_group), :, pl.ds(lane, width)]

    def remote(src, dst, send, recv, peer):
        return pltpu.make_async_remote_copy(
            src_ref=src,
            dst_ref=dst,
            send_sem=send_sem.at[send],
            recv_sem=recv,
            device_id={"tp": peer},
            device_id_type=MESH,
        )

    def sent(send, ref):
        remote(ref, ref, send, tail_sem.at[0], me).wait_send()

    def landed(recv, ref):
        remote(ref, ref, 0, recv, me).wait_recv()

    def owners(index):
        first = index % PREFILL_TP * local_heads
        key = first // heads_here
        return (first * share // heads_here, q_devs + key, q_devs + k_devs + key)

    def proj_from(sender):
        return proj_sem.at[jnp.maximum(sender - (q_devs - 1), 0)]

    def send_proj(peer):
        remote(proj.at[me], proj.at[me], 0, proj_from(me), peer).start()

    def send_projections(urgent):
        for step in range(1, T):
            peer = lax.rem(me + step, T)
            q_owner, k_owner, v_owner = owners(peer)
            hurry = (q_owner == me) | (k_owner == me) | (v_owner == me)
            wanted = hurry if urgent else jnp.logical_not(hurry) & (me >= q_devs)

            @pl.when(wanted)
            def _():
                send_proj(peer)

    def take_proj(sender):
        @pl.when(sender != me)
        def _():
            landed(proj_from(sender), proj.at[sender])

    def push_pages(begin, end):
        for step in range(begin, min(end, T)):
            peer = lax.rem(me + step, T)
            remote(page_stage.at[peer], dec_part(dec, me), 1, tail_sem.at[3], peer).start()

    share_of = -(-(T - 1) // 4)

    def push(send, recv, src):
        for step in range(1, T):
            peer = lax.rem(me + step, T)
            remote(src, src, send, recv, peer).start()

    def take_plane(sems, ref, plane):
        first = plane * plane_size

        @pl.when(plane == my_plane)
        def _():
            landed(sems.at[plane], ref.at[pl.ds(first, plane_size - 1)])

        @pl.when(plane != my_plane)
        def _():
            landed(sems.at[plane], ref.at[pl.ds(first, plane_size)])

    small[2].wait()
    length = column_of(len_ref, B)
    lane = lax.broadcasted_iota(jnp.int32, (B, HEAD_DIM), 1)
    half = HEAD_DIM // 2
    exponent = (lane % half).astype(jnp.float32) * (-2.0 / HEAD_DIM)
    angles = length * jnp.exp(exponent * LOG_BASE)
    turning = jnp.broadcast_to(me < q_devs + k_devs, lane.shape)
    cosine = jnp.where(turning, jnp.cos(angles), 1.0)
    sine = jnp.where(turning, jnp.where(lane < half, -1.0, 1.0) * jnp.sin(angles), 0.0)
    small[3].wait()
    slot_page = lax.broadcasted_iota(jnp.int32, (T, slots), 1) // page_width
    spread = (slot_page == lax.broadcasted_iota(jnp.int32, (T, slots), 0)).astype(jnp.float32)
    inside = lax.broadcasted_iota(jnp.int32, (B, slots), 1) % page_width
    position = jnp.dot(
        table[...].astype(jnp.float32).astype(jnp.bfloat16),
        spread.astype(jnp.bfloat16),
        preferred_element_type=jnp.float32,
    ) * page_width + inside.astype(jnp.float32)
    request_of = lax.broadcasted_iota(jnp.int32, (B, slots), 0)

    def row_at(values, request):
        return jnp.sum(jnp.where(request_of == request, values, 0.0), axis=0, keepdims=True)

    place = [row_at(position, my_group * per_group + e) for e in range(per_group)]
    limit = [
        row_at(jnp.broadcast_to(length, (B, slots)), my_group * per_group + e)
        for e in range(per_group)
    ]
    small[0].wait()
    small[1].wait()
    stream = hid[:, :model]
    normed = normed_by(stream, meansq_of(stream), gain[0:1, :model]).astype(jnp.bfloat16)
    part = jnp.zeros((B, cols), jnp.float32)
    for (lo, hi), piece in zip(cuts, wq_loads):
        piece.wait()
        if hi == model:
            for late in (wo_load, wgu_load, wd_load):
                late.start()
        part = part + dot_t(normed[:, lo:hi], wq[:, lo:hi])
    part = part.astype(jnp.bfloat16).astype(jnp.float32)
    for head in range(heads_here):
        u = part[:, head * HEAD_DIM : (head + 1) * HEAD_DIM]
        swapped = jnp.concatenate([u[:, half:], u[:, :half]], axis=1)
        turned = u * cosine + swapped * sine
        proj[me, :, head * HEAD_DIM : (head + 1) * HEAD_DIM] = turned.astype(jnp.bfloat16)
    pl.semaphore_wait(barrier, T - 1)
    send_projections(True)

    flat_load.wait()
    wanted = lax.broadcasted_iota(jnp.int32, (slots, slots), 0).astype(jnp.float32)
    for e in range(per_group):
        pick = (wanted == place[e]).astype(jnp.float32).astype(jnp.bfloat16)
        for c in range(2):
            moved = jnp.dot(pick, flat[c, e], preferred_element_type=jnp.float32)
            page_stage[:, c, e] = moved.reshape(T, page_width, width).astype(jnp.bfloat16)
    push_pages(1, 1 + share_of)
    q_from, k_from, v_from = owners(me)
    take_proj(q_from)
    take_proj(k_from)

    rows = share * B
    row_of = lax.broadcasted_iota(jnp.int32, (rows, HEAD_DIM), 0)

    def head_of(owner, index):
        at = pl.multiple_of((index % heads_here) * HEAD_DIM, HEAD_DIM)
        return proj[owner, :, pl.ds(at, HEAD_DIM)].astype(jnp.float32)

    found = {}
    for a in range(local_heads):
        kv_head = my_slot * local_heads + a
        q = jnp.concatenate([head_of(q_from, kv_head * share + m) for m in range(share)], axis=0)
        k_new = jnp.concatenate([head_of(k_from, kv_head)] * share, axis=0)
        q16 = q.astype(jnp.bfloat16)
        own = jnp.exp(capped(jnp.sum(q * k_new, axis=-1, keepdims=True) * score_scale))
        lanes = slice(a * HEAD_DIM, (a + 1) * HEAD_DIM)
        for e in range(per_group):
            scores = dot_t(q16, flat[0, e, :, lanes]) * score_scale
            weights = jnp.where(place[e] < limit[e], jnp.exp(capped(scores)), 0.0)
            numer = jnp.dot(
                weights.astype(jnp.bfloat16),
                flat[1, e, :, lanes],
                preferred_element_type=jnp.float32,
            )
            found[a, e] = (numer, jnp.sum(weights, axis=-1, keepdims=True) + own, own)
    take_proj(v_from)
    for a in range(local_heads):
        kv_head = my_slot * local_heads + a
        v_new = jnp.concatenate([head_of(v_from, kv_head)] * share, axis=0)
        picked = [[] for m in range(share)]
        for e in range(per_group):
            request = my_group * per_group + e
            numer, denom, own = found[a, e]
            result = (numer + own.astype(jnp.bfloat16).astype(jnp.float32) * v_new) / denom
            for m in range(share):
                chosen = jnp.where(row_of == m * B + request, result, 0.0)
                picked[m].append(jnp.sum(chosen, axis=0, keepdims=True))
        for m in range(share):
            at = (a * share + m) * HEAD_DIM
            att[me, :, at : at + HEAD_DIM] = jnp.concatenate(picked[m], axis=0).astype(jnp.bfloat16)
    push(2, att_sem.at[my_plane], att.at[me])
    push_pages(1 + share_of, 1 + 2 * share_of)

    first_lane = pl.multiple_of(me * R // LANES * LANES, LANES)
    window = RP + LANES
    turn = window - lax.rem(me * R, LANES)
    own_hid = pltpu.roll(hid[:, pl.ds(first_lane, window)], turn, 1)[:, :RP]
    own_gain = pltpu.roll(gain[:, pl.ds(first_lane, window)], turn, 1)[:, :RP]
    wo_load.wait()
    q_width = att.shape[2]
    halves = T // PREFILL_TP
    slots_half = PREFILL_TP // halves
    half_width = slots_half * q_width
    mixed = jnp.zeros((B, R), jnp.float32)
    for turn_of in range(halves):
        which = (my_plane // (planes // halves) + turn_of) % halves
        for g in range(groups):
            take_plane(att_sem, att, g * halves + which)
        blocks = [
            jnp.concatenate(
                [
                    att[g * PREFILL_TP + which * slots_half + s].astype(jnp.float32)
                    for g in range(groups)
                ],
                axis=0,
            ).astype(jnp.bfloat16)
            for s in range(slots_half)
        ]
        lane_at = pl.multiple_of(which * half_width, half_width)
        mixed = mixed + dot_t(
            jnp.concatenate(blocks, axis=1), wo[:, pl.ds(lane_at, half_width)]
        )
    mixed = mixed.astype(jnp.bfloat16).astype(jnp.float32)
    mixed = jnp.concatenate([mixed, jnp.zeros((B, RP - R), jnp.float32)], axis=1)
    shift = dims["seat_shift"]
    mix[me] = pltpu.roll(mixed, my_seat * shift, 1).astype(jnp.bfloat16)
    push(3, mix_sem.at[my_plane], mix.at[me])
    push_pages(1 + 2 * share_of, 1 + 3 * share_of)
    for step in range(planes):
        take_plane(mix_sem, mix, jnp.int32(step))

    gathered = [None] * chunks
    for s in range(T):
        block = mix[s].astype(jnp.float32)
        for i in range(RP // LANES):
            at = s * R // LANES + i
            tile = block[:, i * LANES : (i + 1) * LANES]
            if at < chunks:
                gathered[at] = tile if gathered[at] is None else gathered[at] + tile
    mixed_all = jnp.concatenate(gathered, axis=1)
    mixed_ms = meansq_of(mixed_all)
    stream = hid[:, :model] + normed_by(mixed_all, mixed_ms, gain[1:2, :model])
    ffn_in = normed_by(stream, meansq_of(stream), gain[2:3, :model]).astype(jnp.bfloat16)
    mine = own_hid + normed_by(mixed, mixed_ms, own_gain[1:2, :])

    push_pages(1 + 3 * share_of, T)
    wgu_load.wait()
    side = ff // 2
    tile = dims["ff_tile"]
    probe = pad_rows(ffn_in, SUBLANES)
    fronts = []
    at_lane = tile // LANES * LANES
    for at in range(0, side, tile):
        flatwise = []
        upright = []
        for c in range(2):
            pushed = jnp.concatenate([wgu[c, at : at + tile, :], probe], axis=0)
            passed = jnp.concatenate([probe, wgu[c, side + at : side + at + tile, :]], axis=0)
            both = dot_t(passed, pushed)
            flatwise.append(both[:B, :tile])
            upright.append(both[SUBLANES:, at_lane:])
        fronts.append(jax.nn.gelu(flatwise[0], approximate=True) * flatwise[1])
        turned_act[at : at + tile, : upright[0].shape[1]] = (
            jax.nn.gelu(upright[0], approximate=True) * upright[1]
        )
    back = turned_act[...].T[tile - at_lane : tile - at_lane + B, :side]
    active = jnp.concatenate(fronts + [back], axis=1).astype(jnp.bfloat16)
    wd_load.wait()
    branch[...] = jnp.dot(active, wd[...], preferred_element_type=jnp.float32).astype(jnp.bfloat16)

    owned = model // owner_count
    span = arrive.shape[2]
    is_owner = (me >= first_owner) & (me < first_owner + owner_count)
    for o in range(owner_count):
        peer = first_owner + o

        @pl.when(me != peer)
        def _():
            piece = branch.at[:, pl.ds(o * owned // LANES * LANES, span)]
            remote(piece, arrive.at[me], 4, tail_sem.at[0], jnp.int32(peer)).start()

    send_projections(False)
    dec_part(dec, me)[...] = page_stage[me]
    landed(tail_sem.at[3], page_stage.at[pl.ds(0, T - 1)])
    for owner in range(q_devs, q_devs + 2 * k_devs):
        @pl.when((owner != k_from) & (owner != v_from))
        def _():
            take_proj(jnp.int32(owner))

    token = lax.broadcasted_iota(jnp.int32, (page_width, cols), 0) + me * page_width
    for c in range(2):
        for i in range(k_devs):
            fresh = proj[q_devs + c * k_devs + i].astype(jnp.float32)
            for r in range(B):
                old = dec[c, r, :, i * cols : (i + 1) * cols].astype(jnp.float32)
                row = jnp.broadcast_to(fresh[r : r + 1, :], old.shape)
                new = jnp.where(token == len_ref[r], row, old)
                dec_done[c, r, :, i * cols : (i + 1) * cols] = new.astype(jnp.bfloat16)

    @pl.when(is_owner)
    def _():
        o = me - first_owner
        odd = o % 2
        base = pl.multiple_of(o * owned // LANES * LANES, LANES)
        total = branch[:, pl.ds(base, span)].astype(jnp.float32)
        landed(tail_sem.at[0], arrive.at[pl.ds(0, T - 1)])
        for s in range(T):
            piece = arrive[s].astype(jnp.float32)
            total = total + jnp.where(me == s, 0.0, piece)
        offset = odd * (LANES // 2)
        lane_of = lax.broadcasted_iota(jnp.int32, (B, span), 1)
        inside = (lane_of >= offset) & (lane_of < offset + owned)
        kept = jnp.where(inside, total, 0.0)
        ready = []
        for i in range(2):
            begin = i * R // LANES * LANES
            left = RP - (i * R - begin) - offset
            ready.append(pltpu.roll(kept[:, begin : begin + RP], lax.rem(left, RP), 1))
            sums[i] = ready[i]
        for i in range(2):
            peer = o * 2 + i

            @pl.when(peer != me)
            def _():
                remote(sums.at[i], sums.at[2], 5, tail_sem.at[1], peer).start()

            @pl.when(peer == me)
            def _():
                sums[2] = ready[i]

        each = jnp.sum(kept * kept, axis=-1, keepdims=True)
        spot = lax.broadcasted_iota(jnp.int32, (B, LANES), 1) == lax.broadcasted_iota(
            jnp.int32, (B, LANES), 0
        )
        squares[o] = jnp.sum(jnp.where(spot, each, 0.0), axis=0, keepdims=True)
        push(6, tail_sem.at[2], squares.at[o])

    for send, ref in ((2, att), (3, mix)):
        sent(send, ref.at[pl.ds(0, T - 1)])
    sent(1, page_stage.at[pl.ds(0, T - 1)])

    @pl.when(me < q_devs)
    def _():
        sent(0, proj.at[0])

    @pl.when(me >= q_devs)
    def _():
        sent(0, proj.at[pl.ds(0, T - 1)])

    @pl.when(is_owner)
    def _():
        sent(4, arrive.at[pl.ds(0, owner_count - 1)])
        landed(tail_sem.at[2], squares.at[pl.ds(0, owner_count - 1)])

    @pl.when(jnp.logical_not(is_owner))
    def _():
        sent(4, arrive.at[pl.ds(0, owner_count)])
        landed(tail_sem.at[2], squares.at[pl.ds(0, owner_count)])

    @pl.when(first_owner + me // 2 != me)
    def _():
        landed(tail_sem.at[1], sums.at[2])

    sumsq = squares[0]
    for s in range(1, owner_count):
        sumsq = sumsq + squares[s]
    spot = lax.broadcasted_iota(jnp.int32, (B, LANES), 1) == lax.broadcasted_iota(
        jnp.int32, (B, LANES), 0
    )
    branch_ms = jnp.sum(
        jnp.where(spot, jnp.broadcast_to(sumsq, (B, LANES)), 0.0), axis=-1, keepdims=True
    ) * (1.0 / model)
    result = mine + normed_by(sums[2], branch_ms, own_gain[3:4, :])
    out_ref[...] = result[:, :R]

    @pl.when(is_owner)
    def _():
        o = me - first_owner
        sent(6, arrive_like(squares, T - 1, owner_count))

        @pl.when(o * 2 == me)
        def _():
            sent(5, sums.at[0])

        @pl.when(o * 2 + 1 == me)
        def _():
            sent(5, sums.at[0])

        @pl.when((o * 2 != me) & (o * 2 + 1 != me))
        def _():
            sent(5, sums.at[pl.ds(0, 2)])


def arrive_like(squares, count, limit):
    return squares.at[pl.ds(0, count)]


def finish_kernel(out_ref, dec_ref, out_hbm, dec_hbm, sem):
    first = pltpu.make_async_copy(dec_ref, dec_hbm, sem.at[0])
    second = pltpu.make_async_copy(out_ref, out_hbm, sem.at[1])
    first.start()
    second.start()
    first.wait()
    second.wait()


def fits_kernel(shapes, devices):
    batch_rows, model = shapes["hidden"]
    cols, rows, ff = shapes["qkv"], shapes["out"], shapes["ff"]
    groups = devices // PREFILL_TP
    weight_bytes = 2 * (cols * model + rows * HEADS * HEAD_DIM + 3 * ff * model)
    return (
        devices == 2 * PREFILL_TP
        and cols == HEADS // PREFILL_TP * HEAD_DIM
        and (KV_HEADS * HEAD_DIM) % cols == 0
        and (HEADS * HEAD_DIM) % cols == 0
        and batch_rows % groups == 0
        and model % (LANES * 2) == 0
        and ff % (6 * SUBLANES) == 0
        and rows * devices == model
        and rows * 4 % LANES == 0
        and weight_bytes < VMEM_LIMIT * 3 // 4
        and batch_rows <= 8
    )


SUBLANES = 16


def fused_device(
    hidden_in,
    prefill_cache,
    lengths,
    page_table,
    qkv_weight,
    out_weight,
    gate_up_weight,
    down_weight,
    norm_gains,
):
    T = lax.axis_size("tp")
    B, model = hidden_in.shape
    groups = T // PREFILL_TP
    per_group = B // groups
    local_heads = KV_HEADS // PREFILL_TP
    share = HEADS // KV_HEADS
    pages, page_width, width = prefill_cache.shape[4:]
    S = pages * page_width
    cols = qkv_weight.shape[1]
    R = out_weight.shape[1]
    RP = -(-R // LANES) * LANES
    ff = down_weight.shape[1]
    k_cols = KV_HEADS * HEAD_DIM
    planes = 4
    plane_size = T // planes
    owner_count = T // 2
    depth = model // 256
    marks = [0, depth // 3, 2 * (depth // 3), depth - 2, depth]
    dims = dict(
        T=T, B=B, R=R, RP=RP, S=S, share=share, local_heads=local_heads,
        per_group=per_group, groups=groups, planes=planes, plane_size=plane_size,
        first_owner=plane_size, owner_count=owner_count, seat_shift=R % LANES,
        cuts=[(lo * 256, hi * 256) for lo, hi in zip(marks, marks[1:])],
        ff_tile=ff // 6,
    )
    q_width = local_heads * share * HEAD_DIM
    span = -(-(model // owner_count) // LANES) * LANES
    bf16, f32 = jnp.bfloat16, jnp.float32
    vmem = pl.BlockSpec(memory_space=pltpu.VMEM)
    anyw = pl.BlockSpec(memory_space=pl.ANY)
    out, dec = pl.pallas_call(
        functools.partial(fused_kernel, dims),
        out_shape=(
            pltpu.VMEM((B, R), f32),
            pltpu.VMEM((2, B, page_width, k_cols), bf16),
        ),
        in_specs=[anyw] * 9,
        out_specs=(vmem, vmem),
        scratch_shapes=[
            pltpu.SMEM((B,), jnp.int32),
            pltpu.VMEM((B, model + RP), f32),
            pltpu.VMEM((norm_gains.shape[1], model + RP), f32),
            pltpu.VMEM((B, T), jnp.int32),
            pltpu.VMEM((2, per_group, S, width), bf16),
            pltpu.VMEM((cols, model), bf16),
            pltpu.VMEM((R, HEADS * HEAD_DIM), bf16),
            pltpu.VMEM((2, ff, model), bf16),
            pltpu.VMEM((ff, model), bf16),
            pltpu.VMEM((T, B, cols), bf16),
            pltpu.VMEM((T, per_group, q_width), bf16),
            pltpu.VMEM((B, HEADS * HEAD_DIM), bf16),
            pltpu.VMEM((T, B, RP), bf16),
            pltpu.VMEM((B, model), bf16),
            pltpu.VMEM((T, B, span), bf16),
            pltpu.VMEM((3, B, RP), f32),
            pltpu.VMEM((T, 1, LANES), f32),
            pltpu.VMEM((-(-ff // (2 * LANES)) * LANES, LANES), f32),
            pltpu.VMEM((T, 2, per_group, page_width, width), bf16),
            pltpu.VMEM((2, B, page_width, k_cols), bf16),
            pltpu.SemaphoreType.DMA((12,)),
            pltpu.SemaphoreType.DMA((7,)),
            pltpu.SemaphoreType.DMA((9,)),
            pltpu.SemaphoreType.DMA((4,)),
            pltpu.SemaphoreType.DMA((4,)),
            pltpu.SemaphoreType.DMA((4,)),
        ],
        compiler_params=pltpu.CompilerParams(
            collective_id=0, has_side_effects=True, vmem_limit_bytes=VMEM_LIMIT
        ),
    )(
        lengths,
        page_table,
        hidden_in,
        norm_gains[0],
        prefill_cache.reshape(2, per_group, S, width),
        qkv_weight[0],
        out_weight[0],
        gate_up_weight[0],
        down_weight[0],
    )
    out, dec = pl.pallas_call(
        finish_kernel,
        out_shape=(
            jax.ShapeDtypeStruct((B, R), f32),
            jax.ShapeDtypeStruct((2, B, page_width, k_cols), bf16),
        ),
        in_specs=[vmem, vmem],
        out_specs=(anyw, anyw),
        scratch_shapes=[pltpu.SemaphoreType.DMA((2,))],
    )(
        pltpu.with_memory_space_constraint(out, pltpu.VMEM),
        pltpu.with_memory_space_constraint(dec, pltpu.VMEM),
    )
    return out, dec.reshape(1, 1, 2, B, page_width, k_cols)


def step(*args):
    shapes = {
        "hidden": args[0].shape,
        "qkv": args[4].shape[1],
        "out": args[5].shape[1],
        "ff": args[7].shape[1],
    }
    chosen = fused_device if fits_kernel(shapes, lax.axis_size("tp")) else on_device
    return chosen(*args)


def solution(mesh):
    placed = (
        P("grp", None),
        P("tp", None, None, "grp", None, None, None),
        P("grp"),
        P("grp", None),
        P(None, "tp", None),
        P(None, "tp", None),
        P(None, None, "tp", None),
        P(None, "tp", None),
        P(),
    )
    return jax.shard_map(
        step,
        mesh=mesh,
        in_specs=placed,
        out_specs=(P("grp", "tp"), P("tp", None, None, "grp", None, None)),
        check_vma=False,
    )
```

```python
import functools

import jax
import jax.numpy as jnp
from jax import lax
from jax.experimental import pallas as pl
from jax.experimental.pallas import tpu as pltpu
from jax.sharding import PartitionSpec as P

D = 4608
HEADS = 32
KV_HEADS = 16
HEAD_DIM = 128
PREFILL_TP = 8


EPSILON = 1e-06
SOFTCAP = 50.0


def rms_scale(vector, gain_row):
    meansq = jnp.mean(vector * vector, axis=-1, keepdims=True)
    return vector * lax.rsqrt(meansq + EPSILON) * (1.0 + gain_row)


def rotate(vector, positions):
    half_dim = vector.shape[-1] // 2
    exponent = jnp.arange(half_dim, dtype=jnp.float32) * (-2.0 / vector.shape[-1])
    frequency = jnp.power(jnp.float32(10000.0), exponent)
    angles = positions.astype(jnp.float32)[:, None, None] * frequency
    cosine = jnp.cos(angles)
    sine_term = jnp.sin(angles)
    front_half = vector[..., :half_dim]
    back_half = vector[..., half_dim:]
    return jnp.concatenate(
        [front_half * cosine - back_half * sine_term, back_half * cosine + front_half * sine_term],
        axis=-1,
    )


def capped(raw_scores):
    return SOFTCAP * jnp.tanh(raw_scores / SOFTCAP)


def round_back(vector):
    return lax.optimization_barrier(vector.astype(jnp.bfloat16)).astype(jnp.float32)


def pick_slot(vector, my_group, my_slot):
    inner = lax.dynamic_index_in_dim(vector, my_group, 0, False)
    return lax.dynamic_index_in_dim(inner, my_slot, 1, False)


def take_pages(page_block, page_order):
    return jnp.take(page_block, page_order, axis=2)


def project_rows(left, weight_rows):
    return jnp.einsum("bd,cd->bc", left, weight_rows, preferred_element_type=jnp.float32)


def on_device(
    hidden_in,
    prefill_cache,
    lengths,
    page_table,
    qkv_weight,
    out_weight,
    gate_up_weight,
    down_weight,
    norm_gains,
):
    devices = lax.axis_size("tp")
    my_index = lax.axis_index("tp")
    batch_rows = hidden_in.shape[0]
    groups = devices // PREFILL_TP
    per_group = batch_rows // groups
    local_heads = KV_HEADS // PREFILL_TP
    head_share = HEADS // KV_HEADS
    layer_count = prefill_cache.shape[1]
    page_width = prefill_cache.shape[5]
    score_scale = (D / HEADS) ** (-0.5)
    q_cols = HEADS * HEAD_DIM
    k_cols = KV_HEADS * HEAD_DIM
    my_group = my_index // PREFILL_TP
    my_slot = my_index % PREFILL_TP
    group_rows = lax.dynamic_slice_in_dim(page_table, my_group * per_group, per_group, 0)
    group_lengths = lax.dynamic_slice_in_dim(lengths, my_group * per_group, per_group, 0)
    local_cache = prefill_cache[0]
    page_ids = jnp.arange(devices, dtype=jnp.int32)
    onehot = (group_rows[:, :, None] == page_ids[None, None, :]).astype(jnp.int32)
    inverse = jnp.sum(onehot * page_ids[None, :, None], axis=1)
    arranged = jax.vmap(take_pages, in_axes=(2, 0), out_axes=2)(local_cache, inverse)
    relaid = lax.all_to_all(arranged, "tp", split_axis=3, concat_axis=3, tiled=True)
    relaid = relaid.reshape(
        layer_count, 2, per_group, groups, PREFILL_TP, page_width, local_heads, HEAD_DIM
    )
    decode_local = relaid.transpose(0, 1, 3, 2, 5, 4, 6, 7).reshape(
        layer_count, 2, batch_rows, page_width, k_cols
    )
    my_pos = my_index * page_width + jnp.arange(page_width, dtype=jnp.int32)
    fresh_slot = my_pos[None, :] == lengths[:, None]
    kept_cache = local_cache.reshape(
        layer_count, 2, per_group, devices, page_width, local_heads, HEAD_DIM
    )
    cache_pos = (
        group_rows[:, :, None] * page_width + jnp.arange(page_width, dtype=jnp.int32)[None, None, :]
    )
    kept_visible = cache_pos < group_lengths[:, None, None]
    stream = hidden_in
    normed = rms_scale(stream, norm_gains[0, 0]).astype(jnp.bfloat16)
    column_part = project_rows(normed, qkv_weight[0]).astype(jnp.bfloat16)
    projected = lax.all_gather(column_part, "tp", axis=1, tiled=True)
    queries = rotate(
        projected[:, :q_cols].astype(jnp.float32).reshape(batch_rows, HEADS, HEAD_DIM), lengths
    ).astype(jnp.bfloat16)
    new_key = rotate(
        projected[:, q_cols : q_cols + k_cols]
        .astype(jnp.float32)
        .reshape(batch_rows, KV_HEADS, HEAD_DIM),
        lengths,
    ).astype(jnp.bfloat16)
    new_value = projected[:, q_cols + k_cols :]
    key_layer = jnp.where(
        fresh_slot[:, :, None], new_key.reshape(batch_rows, 1, k_cols), decode_local[0, 0]
    )
    value_layer = jnp.where(
        fresh_slot[:, :, None], new_value.reshape(batch_rows, 1, k_cols), decode_local[0, 1]
    )
    written = [jnp.stack([key_layer, value_layer], axis=0)]
    flat_q = queries.reshape(batch_rows, KV_HEADS, head_share, HEAD_DIM)
    flat_k = new_key.reshape(batch_rows, KV_HEADS, 1, HEAD_DIM)
    flat_v = new_value.reshape(batch_rows, KV_HEADS, 1, HEAD_DIM)
    own_weight = jnp.exp(
        capped(
            jnp.sum(flat_q.astype(jnp.float32) * flat_k.astype(jnp.float32), axis=-1) * score_scale
        )
    )
    own_term = round_back(own_weight)[..., None] * flat_v.astype(jnp.float32)
    shaped_q = flat_q.reshape(groups, per_group, PREFILL_TP, local_heads, head_share, HEAD_DIM)
    shaped_own = own_weight.reshape(groups, per_group, PREFILL_TP, local_heads, head_share)
    shaped_term = own_term.reshape(groups, per_group, PREFILL_TP, local_heads, head_share, HEAD_DIM)
    my_queries = pick_slot(shaped_q, my_group, my_slot)
    cached_keys = kept_cache[0, 0]
    cached_values = kept_cache[0, 1]
    raw_scores = (
        jnp.einsum("ramd,rjcad->ramjc", my_queries, cached_keys, preferred_element_type=jnp.float32)
        * score_scale
    )
    weights = jnp.where(kept_visible[:, None, None, :, :], jnp.exp(capped(raw_scores)), 0.0)
    numerator = jnp.einsum(
        "ramjc,rjcad->ramd",
        weights.astype(jnp.bfloat16),
        cached_values,
        preferred_element_type=jnp.float32,
    )
    numerator = numerator + pick_slot(shaped_term, my_group, my_slot)
    denominator = jnp.sum(weights, axis=(-2, -1)) + pick_slot(shaped_own, my_group, my_slot)
    mine = (
        (numerator / denominator[..., None])
        .astype(jnp.bfloat16)
        .reshape(1, per_group, local_heads * head_share * HEAD_DIM)
    )
    gathered = lax.all_gather(mine, "tp", axis=0, tiled=True)
    attended = (
        gathered.reshape(groups, PREFILL_TP, per_group, local_heads * head_share * HEAD_DIM)
        .transpose(0, 2, 1, 3)
        .reshape(batch_rows, q_cols)
    )
    mixed_part = project_rows(attended, out_weight[0]).astype(jnp.bfloat16)
    mixed_out = lax.all_gather(mixed_part, "tp", axis=1, tiled=True)
    stream = stream + rms_scale(mixed_out.astype(jnp.float32), norm_gains[0, 1])
    ffn_in = rms_scale(stream, norm_gains[0, 2]).astype(jnp.bfloat16)
    gate_proj = project_rows(ffn_in, gate_up_weight[0, 0])
    up_proj = project_rows(ffn_in, gate_up_weight[0, 1])
    active = (jax.nn.gelu(gate_proj, approximate=True) * up_proj).astype(jnp.bfloat16)
    branch = jnp.dot(active, down_weight[0], preferred_element_type=jnp.float32)
    column_count = branch.shape[1] // devices
    summed = lax.psum(branch, "tp")
    stream = stream + rms_scale(summed, norm_gains[0, 3])
    result = lax.dynamic_slice_in_dim(stream, my_index * column_count, column_count, 1)
    decode_cache = jnp.stack(written, axis=0)[None]
    return (result, decode_cache)


MESH = pl.DeviceIdType.MESH
LANES = 128
NT = (((1,), (1,)), ((), ()))
LOG_BASE = 9.210340371976184
UNROLL = True
VMEM_LIMIT = 58 * 1024 * 1024


def dot_t(left, right):
    return lax.dot_general(left, right, NT, preferred_element_type=jnp.float32)


def normed_by(vector, meansq, gain):
    return vector * lax.rsqrt(meansq + EPSILON) * (1.0 + gain)


def meansq_of(vector):
    return jnp.mean(vector * vector, axis=-1, keepdims=True)


def column_of(scalars, count):
    row = lax.broadcasted_iota(jnp.int32, (count, 1), 0)
    column = jnp.zeros((count, 1), jnp.int32)
    for i in range(count):
        column = jnp.where(row == i, scalars[i], column)
    return column.astype(jnp.float32)


def pad_rows(rows, count):
    return jnp.concatenate(
        [rows, jnp.zeros((count - rows.shape[0], rows.shape[1]), rows.dtype)], axis=0
    )


def fused_kernel(
    dims,
    len_hbm,
    table_hbm,
    hid_hbm,
    gain_hbm,
    flat_hbm,
    wq_hbm,
    wo_hbm,
    wgu_hbm,
    wd_hbm,
    out_ref,
    dec_done,
    len_ref,
    hid,
    gain,
    table,
    flat,
    wq,
    wo,
    wgu,
    wd,
    proj,
    att,
    attended,
    mix,
    branch,
    arrive,
    sums,
    squares,
    stack,
    mixed_ref,
    blend,
    page_stage,
    dec,
    load_sem,
    send_sem,
    proj_sem,
    att_sem,
    mix_sem,
    tail_sem,
):
    T, B, R, RP = dims["T"], dims["B"], dims["R"], dims["RP"]
    share, local_heads, slots = dims["share"], dims["local_heads"], dims["S"]
    per_group, groups = dims["per_group"], dims["groups"]
    planes, plane_size = dims["planes"], dims["plane_size"]
    first_owner, owner_count = dims["first_owner"], dims["owner_count"]
    width = local_heads * HEAD_DIM
    cols = wq.shape[0]
    heads_here = cols // HEAD_DIM
    q_devs = HEADS * HEAD_DIM // cols
    k_devs = KV_HEADS * HEAD_DIM // cols
    page_width = dec.shape[2]
    model = wq.shape[1]
    ff = wd.shape[0]
    chunks = model // LANES
    score_scale = (D / HEADS) ** (-0.5)
    me = lax.axis_index("tp")
    my_group = me // PREFILL_TP
    my_slot = me % PREFILL_TP
    my_plane = me // plane_size
    my_seat = me % plane_size

    def load(index, src, dst):
        return pltpu.make_async_copy(src, dst, load_sem.at[index])

    small = [
        load(0, hid_hbm, hid.at[:, pl.ds(0, model)]),
        load(1, gain_hbm, gain.at[:, pl.ds(0, model)]),
        load(2, len_hbm, len_ref),
        load(3, table_hbm, table),
    ]
    cuts = dims["cuts"]
    wq_loads = [
        load(8 + i, wq_hbm.at[:, pl.ds(lo, hi - lo)], wq.at[:, pl.ds(lo, hi - lo)])
        for i, (lo, hi) in enumerate(cuts)
    ]
    flat_load = load(4, flat_hbm, flat)
    wo_load = load(5, wo_hbm, wo)
    wgu_load = load(6, wgu_hbm, wgu)
    wd_load = load(7, wd_hbm, wd)
    for piece in small + wq_loads + [flat_load]:
        piece.start()

    barrier = pltpu.get_barrier_semaphore()

    def greet(step, carry):
        peer = lax.rem(me + step, T)
        pl.semaphore_signal(barrier, inc=1, device_id={"tp": peer}, device_id_type=MESH)
        return carry

    lax.fori_loop(1, T, greet, 0)

    def dec_part(ref, index):
        group, slot = index // PREFILL_TP, index % PREFILL_TP
        lane = pl.multiple_of(slot * width, width)
        return ref.at[:, pl.ds(group * per_group, per_group), :, pl.ds(lane, width)]

    def remote(src, dst, send, recv, peer):
        return pltpu.make_async_remote_copy(
            src_ref=src,
            dst_ref=dst,
            send_sem=send_sem.at[send],
            recv_sem=recv,
            device_id={"tp": peer},
            device_id_type=MESH,
        )

    def sent(send, ref):
        remote(ref, ref, send, tail_sem.at[0], me).wait_send()

    def landed(recv, ref):
        remote(ref, ref, 0, recv, me).wait_recv()

    def owners(index):
        first = index % PREFILL_TP * local_heads
        key = first // heads_here
        return (first * share // heads_here, q_devs + key, q_devs + k_devs + key)

    def proj_from(sender):
        return proj_sem.at[jnp.maximum(sender - (q_devs - 1), 0)]

    def send_proj(peer):
        remote(proj.at[me], proj.at[me], 0, proj_from(me), peer).start()

    def send_projections(urgent):
        for step in range(1, T):
            peer = lax.rem(me + step, T)
            q_owner, k_owner, v_owner = owners(peer)
            hurry = (q_owner == me) | (k_owner == me) | (v_owner == me)
            wanted = hurry if urgent else jnp.logical_not(hurry) & (me >= q_devs)

            @pl.when(wanted)
            def _():
                send_proj(peer)

    def take_proj(sender):
        @pl.when(sender != me)
        def _():
            landed(proj_from(sender), proj.at[sender])

    def push_pages(begin, end):
        for step in range(begin, min(end, T)):
            peer = lax.rem(me + step, T)
            remote(page_stage.at[peer], dec_part(dec, me), 1, tail_sem.at[3], peer).start()

    def push(send, recv, src):
        for step in range(1, T):
            peer = lax.rem(me + step, T)
            remote(src, src, send, recv, peer).start()

    def take_plane(sems, ref, plane):
        first = plane * plane_size

        @pl.when(plane == my_plane)
        def _():
            landed(sems.at[plane], ref.at[pl.ds(first, plane_size - 1)])

        @pl.when(plane != my_plane)
        def _():
            landed(sems.at[plane], ref.at[pl.ds(first, plane_size)])

    small[2].wait()
    length = column_of(len_ref, B)
    lane = lax.broadcasted_iota(jnp.int32, (B, HEAD_DIM), 1)
    half = HEAD_DIM // 2
    exponent = (lane % half).astype(jnp.float32) * (-2.0 / HEAD_DIM)
    angles = length * jnp.exp(exponent * LOG_BASE)
    turning = jnp.broadcast_to(me < q_devs + k_devs, lane.shape)
    cosine = jnp.where(turning, jnp.cos(angles), 1.0)
    sine = jnp.where(turning, jnp.where(lane < half, -1.0, 1.0) * jnp.sin(angles), 0.0)
    small[3].wait()
    slot_page = lax.broadcasted_iota(jnp.int32, (T, slots), 1) // page_width
    spread = (slot_page == lax.broadcasted_iota(jnp.int32, (T, slots), 0)).astype(jnp.float32)
    inside = lax.broadcasted_iota(jnp.int32, (B, slots), 1) % page_width
    position = jnp.dot(
        table[...].astype(jnp.float32).astype(jnp.bfloat16),
        spread.astype(jnp.bfloat16),
        preferred_element_type=jnp.float32,
    ) * page_width + inside.astype(jnp.float32)
    request_of = lax.broadcasted_iota(jnp.int32, (B, slots), 0)

    def row_at(values, request):
        return jnp.sum(jnp.where(request_of == request, values, 0.0), axis=0, keepdims=True)

    place = [row_at(position, my_group * per_group + e) for e in range(per_group)]
    limit = [
        row_at(jnp.broadcast_to(length, (B, slots)), my_group * per_group + e)
        for e in range(per_group)
    ]
    small[0].wait()
    small[1].wait()
    stream = hid[:, :model]
    normed = normed_by(stream, meansq_of(stream), gain[0:1, :model]).astype(jnp.bfloat16)
    part = jnp.zeros((B, cols), jnp.float32)
    for (lo, hi), piece in zip(cuts, wq_loads):
        piece.wait()
        if hi == model:
            for late in (wo_load, wgu_load, wd_load):
                late.start()
        part = part + dot_t(normed[:, lo:hi], wq[:, lo:hi])
    part = part.astype(jnp.bfloat16).astype(jnp.float32)
    for head in range(heads_here):
        u = part[:, head * HEAD_DIM : (head + 1) * HEAD_DIM]
        swapped = jnp.concatenate([u[:, half:], u[:, :half]], axis=1)
        turned = u * cosine + swapped * sine
        proj[me, :, head * HEAD_DIM : (head + 1) * HEAD_DIM] = turned.astype(jnp.bfloat16)
    pl.semaphore_wait(barrier, T - 1)
    send_projections(True)

    flat_load.wait()
    wanted = lax.broadcasted_iota(jnp.int32, (slots, slots), 0).astype(jnp.float32)
    for e in range(per_group):
        pick = (wanted == place[e]).astype(jnp.float32).astype(jnp.bfloat16)
        for c in range(2):
            moved = jnp.dot(pick, flat[c, e], preferred_element_type=jnp.float32)
            page_stage[:, c, e] = moved.reshape(T, page_width, width).astype(jnp.bfloat16)
    push_pages(1, dims["page_cut"])
    q_from, k_from, v_from = owners(me)
    take_proj(q_from)
    take_proj(k_from)

    rows = share * B
    row_of = lax.broadcasted_iota(jnp.int32, (rows, HEAD_DIM), 0)

    def head_of(owner, index):
        at = pl.multiple_of((index % heads_here) * HEAD_DIM, HEAD_DIM)
        return proj[owner, :, pl.ds(at, HEAD_DIM)].astype(jnp.float32)

    found = {}
    for a in range(local_heads):
        kv_head = my_slot * local_heads + a
        q = jnp.concatenate([head_of(q_from, kv_head * share + m) for m in range(share)], axis=0)
        k_new = jnp.concatenate([head_of(k_from, kv_head)] * share, axis=0)
        q16 = q.astype(jnp.bfloat16)
        own = jnp.exp(capped(jnp.sum(q * k_new, axis=-1, keepdims=True) * score_scale))
        lanes = slice(a * HEAD_DIM, (a + 1) * HEAD_DIM)
        for e in range(per_group):
            scores = dot_t(q16, flat[0, e, :, lanes]) * score_scale
            weights = jnp.where(place[e] < limit[e], jnp.exp(capped(scores)), 0.0)
            numer = jnp.dot(
                weights.astype(jnp.bfloat16),
                flat[1, e, :, lanes],
                preferred_element_type=jnp.float32,
            )
            found[a, e] = (numer, jnp.sum(weights, axis=-1, keepdims=True) + own, own)
    take_proj(v_from)
    for a in range(local_heads):
        kv_head = my_slot * local_heads + a
        v_new = jnp.concatenate([head_of(v_from, kv_head)] * share, axis=0)
        picked = [[] for m in range(share)]
        for e in range(per_group):
            request = my_group * per_group + e
            numer, denom, own = found[a, e]
            result = (numer + own.astype(jnp.bfloat16).astype(jnp.float32) * v_new) / denom
            for m in range(share):
                chosen = jnp.where(row_of == m * B + request, result, 0.0)
                picked[m].append(jnp.sum(chosen, axis=0, keepdims=True))
        for m in range(share):
            at = (a * share + m) * HEAD_DIM
            att[me, :, at : at + HEAD_DIM] = jnp.concatenate(picked[m], axis=0).astype(jnp.bfloat16)
    push(2, att_sem.at[my_plane], att.at[me])

    first_lane = pl.multiple_of(me * R // LANES * LANES, LANES)
    window = RP + LANES
    turn = window - lax.rem(me * R, LANES)
    own_hid = pltpu.roll(hid[:, pl.ds(first_lane, window)], turn, 1)[:, :RP]
    own_gain = pltpu.roll(gain[:, pl.ds(first_lane, window)], turn, 1)[:, :RP]
    wo_load.wait()
    q_width = att.shape[2]
    halves = T // PREFILL_TP
    slots_half = PREFILL_TP // halves
    half_width = slots_half * q_width
    mixed = jnp.zeros((B, R), jnp.float32)
    for turn_of in range(halves):
        which = (my_plane // (planes // halves) + turn_of) % halves
        for g in range(groups):
            take_plane(att_sem, att, g * halves + which)
        blocks = [
            jnp.concatenate(
                [
                    att[g * PREFILL_TP + which * slots_half + s].astype(jnp.float32)
                    for g in range(groups)
                ],
                axis=0,
            ).astype(jnp.bfloat16)
            for s in range(slots_half)
        ]
        lane_at = pl.multiple_of(which * half_width, half_width)
        mixed = mixed + dot_t(
            jnp.concatenate(blocks, axis=1), wo[:, pl.ds(lane_at, half_width)]
        )
    mixed = mixed.astype(jnp.bfloat16).astype(jnp.float32)
    mixed = jnp.concatenate([mixed, jnp.zeros((B, RP - R), jnp.float32)], axis=1)
    shift = dims["seat_shift"]
    mix[me] = pltpu.roll(mixed, my_seat * shift, 1).astype(jnp.bfloat16)
    push(3, mix_sem.at[my_plane], mix.at[me])
    blend[:B, :] = hid[:, :model] * (1.0 + gain[2:3, :model])
    wgu_load.wait()
    side = ff // 2
    tile = dims["ff_tile"]
    at_lane = tile // LANES * LANES
    blocks = [(s, c) for s in range(side // tile) for c in range(2)]
    half_cols = model // halves
    half_seats = T // halves
    front, upright = {}, {}
    for turn_of in range(halves):
        which = (my_plane // (planes // halves) + turn_of) % halves
        for p in range(planes // halves):
            plane = which * (planes // halves) + p
            if turn_of:
                landed(mix_sem.at[plane], mix.at[pl.ds(plane * plane_size, plane_size)])
            else:
                take_plane(mix_sem, mix, plane)
        if turn_of == 0:
            push_pages(dims["page_cut"], T)
            send_projections(False)
        tiles = [None] * (half_cols // LANES)
        for s in range(half_seats):
            block = mix[which * half_seats + s].astype(jnp.float32)
            for i in range(RP // LANES):
                at = s * R // LANES + i
                piece = block[:, i * LANES : (i + 1) * LANES]
                if at < len(tiles):
                    tiles[at] = piece if tiles[at] is None else tiles[at] + piece
        got = jnp.concatenate(tiles, axis=1)
        span_at = pl.ds(pl.multiple_of(which * half_cols, LANES), half_cols)
        mixed_ref[:, span_at] = got
        blend[B:, span_at] = got * ((1.0 + gain[1:2, span_at]) * (1.0 + gain[2:3, span_at]))
        exact = blend[:, span_at]
        high = exact.astype(jnp.bfloat16).astype(jnp.float32)
        probe = jnp.concatenate([high, exact - high], axis=0).astype(jnp.bfloat16)
        if turn_of == halves - 1:
            mixed_all = mixed_ref[...]
            mixed_ms = meansq_of(mixed_all)
            stream = hid[:, :model] + normed_by(mixed_all, mixed_ms, gain[1:2, :model])
            outer = lax.rsqrt(meansq_of(stream) + EPSILON)
            inner = lax.rsqrt(mixed_ms + EPSILON)
            mine = own_hid + normed_by(mixed, mixed_ms, own_gain[1:2, :])
        for s, c in blocks:
            at = s * tile
            pushed = jnp.concatenate([wgu[c, at : at + tile, span_at], probe], axis=0)
            passed = jnp.concatenate(
                [probe, wgu[c, side + at : side + at + tile, span_at]], axis=0
            )
            both = dot_t(passed, pushed)
            part = both[: 2 * B, :tile] + both[2 * B : 4 * B, :tile]
            front[s, c] = part if turn_of == 0 else front[s, c] + part
            rest = both[4 * B :, at_lane:]
            wide = rest.shape[1]
            if turn_of < halves - 1:
                stack[s, c, :, :wide] = rest
            else:
                rest = jnp.concatenate(
                    [rest + stack[s, c, :, :wide], jnp.zeros((tile, LANES - wide), jnp.float32)],
                    axis=1,
                )
                turned = rest.T
                first = tile - at_lane
                upright[s, c] = turned[first : first + 2 * B] + turned[first + 2 * B : first + 4 * B]

    def settle(parts):
        return outer * (parts[:B] + inner * parts[B:])

    steps = range(side // tile)
    active = []
    for table_of in (front, upright):
        for s in steps:
            gate, up = settle(table_of[s, 0]), settle(table_of[s, 1])
            active.append(jax.nn.gelu(gate, approximate=True) * up)
    active = jnp.concatenate(active, axis=1).astype(jnp.bfloat16)
    wd_load.wait()
    branch[...] = jnp.dot(active, wd[...], preferred_element_type=jnp.float32).astype(jnp.bfloat16)

    owned = model // owner_count
    span = arrive.shape[2]
    is_owner = (me >= first_owner) & (me < first_owner + owner_count)
    for o in range(owner_count):
        peer = first_owner + o

        @pl.when(me != peer)
        def _():
            piece = branch.at[:, pl.ds(o * owned // LANES * LANES, span)]
            remote(piece, arrive.at[me], 4, tail_sem.at[0], jnp.int32(peer)).start()

    @pl.when(is_owner)
    def _():
        o = me - first_owner
        odd = o % 2
        base = pl.multiple_of(o * owned // LANES * LANES, LANES)
        total = branch[:, pl.ds(base, span)].astype(jnp.float32)
        landed(tail_sem.at[0], arrive.at[pl.ds(0, T - 1)])
        for s in range(T):
            piece = arrive[s].astype(jnp.float32)
            total = total + jnp.where(me == s, 0.0, piece)
        offset = odd * (LANES // 2)
        lane_of = lax.broadcasted_iota(jnp.int32, (B, span), 1)
        inside = (lane_of >= offset) & (lane_of < offset + owned)
        kept = jnp.where(inside, total, 0.0)
        ready = []
        for i in range(2):
            begin = i * R // LANES * LANES
            left = RP - (i * R - begin) - offset
            ready.append(pltpu.roll(kept[:, begin : begin + RP], lax.rem(left, RP), 1))
            sums[i] = ready[i]
        for i in range(2):
            peer = o * 2 + i

            @pl.when(peer != me)
            def _():
                remote(sums.at[i], sums.at[2], 5, tail_sem.at[1], peer).start()

            @pl.when(peer == me)
            def _():
                sums[2] = ready[i]

        each = jnp.sum(kept * kept, axis=-1, keepdims=True)
        spot = lax.broadcasted_iota(jnp.int32, (B, LANES), 1) == lax.broadcasted_iota(
            jnp.int32, (B, LANES), 0
        )
        squares[o] = jnp.sum(jnp.where(spot, each, 0.0), axis=0, keepdims=True)
        push(6, tail_sem.at[2], squares.at[o])

    dec_part(dec, me)[...] = page_stage[me]
    landed(tail_sem.at[3], page_stage.at[pl.ds(0, T - 1)])
    for owner in range(q_devs, q_devs + 2 * k_devs):
        @pl.when((owner != k_from) & (owner != v_from))
        def _():
            take_proj(jnp.int32(owner))

    token = lax.broadcasted_iota(jnp.int32, (page_width, cols), 0) + me * page_width
    for c in range(2):
        for i in range(k_devs):
            fresh = proj[q_devs + c * k_devs + i].astype(jnp.float32)
            for r in range(B):
                old = dec[c, r, :, i * cols : (i + 1) * cols].astype(jnp.float32)
                row = jnp.broadcast_to(fresh[r : r + 1, :], old.shape)
                new = jnp.where(token == len_ref[r], row, old)
                dec_done[c, r, :, i * cols : (i + 1) * cols] = new.astype(jnp.bfloat16)

    for send, ref in ((2, att), (3, mix)):
        sent(send, ref.at[pl.ds(0, T - 1)])
    sent(1, page_stage.at[pl.ds(0, T - 1)])

    @pl.when(me < q_devs)
    def _():
        sent(0, proj.at[0])

    @pl.when(me >= q_devs)
    def _():
        sent(0, proj.at[pl.ds(0, T - 1)])

    @pl.when(is_owner)
    def _():
        sent(4, arrive.at[pl.ds(0, owner_count - 1)])
        landed(tail_sem.at[2], squares.at[pl.ds(0, owner_count - 1)])

    @pl.when(jnp.logical_not(is_owner))
    def _():
        sent(4, arrive.at[pl.ds(0, owner_count)])
        landed(tail_sem.at[2], squares.at[pl.ds(0, owner_count)])

    @pl.when(first_owner + me // 2 != me)
    def _():
        landed(tail_sem.at[1], sums.at[2])

    sumsq = squares[0]
    for s in range(1, owner_count):
        sumsq = sumsq + squares[s]
    spot = lax.broadcasted_iota(jnp.int32, (B, LANES), 1) == lax.broadcasted_iota(
        jnp.int32, (B, LANES), 0
    )
    branch_ms = jnp.sum(
        jnp.where(spot, jnp.broadcast_to(sumsq, (B, LANES)), 0.0), axis=-1, keepdims=True
    ) * (1.0 / model)
    result = mine + normed_by(sums[2], branch_ms, own_gain[3:4, :])
    out_ref[...] = result[:, :R]

    @pl.when(is_owner)
    def _():
        o = me - first_owner
        sent(6, arrive_like(squares, T - 1, owner_count))

        @pl.when(o * 2 == me)
        def _():
            sent(5, sums.at[0])

        @pl.when(o * 2 + 1 == me)
        def _():
            sent(5, sums.at[0])

        @pl.when((o * 2 != me) & (o * 2 + 1 != me))
        def _():
            sent(5, sums.at[pl.ds(0, 2)])


def arrive_like(squares, count, limit):
    return squares.at[pl.ds(0, count)]


def finish_kernel(out_ref, dec_ref, out_hbm, dec_hbm, sem):
    first = pltpu.make_async_copy(dec_ref, dec_hbm, sem.at[0])
    second = pltpu.make_async_copy(out_ref, out_hbm, sem.at[1])
    first.start()
    second.start()
    first.wait()
    second.wait()


def fits_kernel(shapes, devices):
    batch_rows, model = shapes["hidden"]
    cols, rows, ff = shapes["qkv"], shapes["out"], shapes["ff"]
    groups = devices // PREFILL_TP
    weight_bytes = 2 * (cols * model + rows * HEADS * HEAD_DIM + 3 * ff * model)
    return (
        devices == 2 * PREFILL_TP
        and cols == HEADS // PREFILL_TP * HEAD_DIM
        and (KV_HEADS * HEAD_DIM) % cols == 0
        and (HEADS * HEAD_DIM) % cols == 0
        and batch_rows % groups == 0
        and model % (LANES * 2) == 0
        and ff % (6 * SUBLANES) == 0
        and rows * devices == model
        and rows * 4 % LANES == 0
        and weight_bytes < VMEM_LIMIT * 3 // 4
        and batch_rows == 4
    )


SUBLANES = 16


def fused_device(
    hidden_in,
    prefill_cache,
    lengths,
    page_table,
    qkv_weight,
    out_weight,
    gate_up_weight,
    down_weight,
    norm_gains,
):
    T = lax.axis_size("tp")
    B, model = hidden_in.shape
    groups = T // PREFILL_TP
    per_group = B // groups
    local_heads = KV_HEADS // PREFILL_TP
    share = HEADS // KV_HEADS
    pages, page_width, width = prefill_cache.shape[4:]
    S = pages * page_width
    cols = qkv_weight.shape[1]
    R = out_weight.shape[1]
    RP = -(-R // LANES) * LANES
    ff = down_weight.shape[1]
    k_cols = KV_HEADS * HEAD_DIM
    planes = 4
    plane_size = T // planes
    owner_count = T // 2
    depth = model // 256
    marks = list(range(0, depth, 2)) + [depth]
    dims = dict(
        T=T, B=B, R=R, RP=RP, S=S, share=share, local_heads=local_heads,
        per_group=per_group, groups=groups, planes=planes, plane_size=plane_size,
        first_owner=plane_size, owner_count=owner_count, seat_shift=R % LANES,
        cuts=[(lo * 256, hi * 256) for lo, hi in zip(marks, marks[1:])],
        ff_tile=ff // 6, page_cut=T // 2,
    )
    q_width = local_heads * share * HEAD_DIM
    span = -(-(model // owner_count) // LANES) * LANES
    bf16, f32 = jnp.bfloat16, jnp.float32
    vmem = pl.BlockSpec(memory_space=pltpu.VMEM)
    anyw = pl.BlockSpec(memory_space=pl.ANY)
    out, dec = pl.pallas_call(
        functools.partial(fused_kernel, dims),
        out_shape=(
            pltpu.VMEM((B, R), f32),
            pltpu.VMEM((2, B, page_width, k_cols), bf16),
        ),
        in_specs=[anyw] * 9,
        out_specs=(vmem, vmem),
        scratch_shapes=[
            pltpu.SMEM((B,), jnp.int32),
            pltpu.VMEM((B, model + RP), f32),
            pltpu.VMEM((norm_gains.shape[1], model + RP), f32),
            pltpu.VMEM((B, T), jnp.int32),
            pltpu.VMEM((2, per_group, S, width), bf16),
            pltpu.VMEM((cols, model), bf16),
            pltpu.VMEM((R, HEADS * HEAD_DIM), bf16),
            pltpu.VMEM((2, ff, model), bf16),
            pltpu.VMEM((ff, model), bf16),
            pltpu.VMEM((T, B, cols), bf16),
            pltpu.VMEM((T, per_group, q_width), bf16),
            pltpu.VMEM((B, HEADS * HEAD_DIM), bf16),
            pltpu.VMEM((T, B, RP), bf16),
            pltpu.VMEM((B, model), bf16),
            pltpu.VMEM((T, B, span), bf16),
            pltpu.VMEM((3, B, RP), f32),
            pltpu.VMEM((T, 1, LANES), f32),
            pltpu.VMEM((3, 2, ff // 6, LANES), f32),
            pltpu.VMEM((B, model), f32),
            pltpu.VMEM((2 * B, model), f32),
            pltpu.VMEM((T, 2, per_group, page_width, width), bf16),
            pltpu.VMEM((2, B, page_width, k_cols), bf16),
            pltpu.SemaphoreType.DMA((8 + len(dims["cuts"]),)),
            pltpu.SemaphoreType.DMA((7,)),
            pltpu.SemaphoreType.DMA((9,)),
            pltpu.SemaphoreType.DMA((4,)),
            pltpu.SemaphoreType.DMA((4,)),
            pltpu.SemaphoreType.DMA((4,)),
        ],
        compiler_params=pltpu.CompilerParams(
            collective_id=0, has_side_effects=True, vmem_limit_bytes=VMEM_LIMIT
        ),
    )(
        lengths,
        page_table,
        hidden_in,
        norm_gains[0],
        prefill_cache.reshape(2, per_group, S, width),
        qkv_weight[0],
        out_weight[0],
        gate_up_weight[0],
        down_weight[0],
    )
    out, dec = pl.pallas_call(
        finish_kernel,
        out_shape=(
            jax.ShapeDtypeStruct((B, R), f32),
            jax.ShapeDtypeStruct((2, B, page_width, k_cols), bf16),
        ),
        in_specs=[vmem, vmem],
        out_specs=(anyw, anyw),
        scratch_shapes=[pltpu.SemaphoreType.DMA((2,))],
    )(
        pltpu.with_memory_space_constraint(out, pltpu.VMEM),
        pltpu.with_memory_space_constraint(dec, pltpu.VMEM),
    )
    return out, dec.reshape(1, 1, 2, B, page_width, k_cols)


def step(*args):
    shapes = {
        "hidden": args[0].shape,
        "qkv": args[4].shape[1],
        "out": args[5].shape[1],
        "ff": args[7].shape[1],
    }
    chosen = fused_device if fits_kernel(shapes, lax.axis_size("tp")) else on_device
    return chosen(*args)


def solution(mesh):
    placed = (
        P("grp", None),
        P("tp", None, None, "grp", None, None, None),
        P("grp"),
        P("grp", None),
        P(None, "tp", None),
        P(None, "tp", None),
        P(None, None, "tp", None),
        P(None, "tp", None),
        P(),
    )
    return jax.shard_map(
        step,
        mesh=mesh,
        in_specs=placed,
        out_specs=(P("grp", "tp"), P("tp", None, None, "grp", None, None)),
        check_vma=False,
    )
```

```python
import functools

import jax
import jax.numpy as jnp
from jax import lax
from jax.experimental import pallas as pl
from jax.experimental.pallas import tpu as pltpu
from jax.sharding import PartitionSpec as P

D = 4608
HEADS = 32
KV_HEADS = 16
HEAD_DIM = 128
PREFILL_TP = 8


EPSILON = 1e-06
SOFTCAP = 50.0


def rms_scale(vector, gain_row):
    meansq = jnp.mean(vector * vector, axis=-1, keepdims=True)
    return vector * lax.rsqrt(meansq + EPSILON) * (1.0 + gain_row)


def rotate(vector, positions):
    half_dim = vector.shape[-1] // 2
    exponent = jnp.arange(half_dim, dtype=jnp.float32) * (-2.0 / vector.shape[-1])
    frequency = jnp.power(jnp.float32(10000.0), exponent)
    angles = positions.astype(jnp.float32)[:, None, None] * frequency
    cosine = jnp.cos(angles)
    sine_term = jnp.sin(angles)
    front_half = vector[..., :half_dim]
    back_half = vector[..., half_dim:]
    return jnp.concatenate(
        [front_half * cosine - back_half * sine_term, back_half * cosine + front_half * sine_term],
        axis=-1,
    )


def capped(raw_scores):
    return SOFTCAP * jnp.tanh(raw_scores / SOFTCAP)


def round_back(vector):
    return lax.optimization_barrier(vector.astype(jnp.bfloat16)).astype(jnp.float32)


def pick_slot(vector, my_group, my_slot):
    inner = lax.dynamic_index_in_dim(vector, my_group, 0, False)
    return lax.dynamic_index_in_dim(inner, my_slot, 1, False)


def take_pages(page_block, page_order):
    return jnp.take(page_block, page_order, axis=2)


def project_rows(left, weight_rows):
    return jnp.einsum("bd,cd->bc", left, weight_rows, preferred_element_type=jnp.float32)


def on_device(
    hidden_in,
    prefill_cache,
    lengths,
    page_table,
    qkv_weight,
    out_weight,
    gate_up_weight,
    down_weight,
    norm_gains,
):
    devices = lax.axis_size("tp")
    my_index = lax.axis_index("tp")
    batch_rows = hidden_in.shape[0]
    groups = devices // PREFILL_TP
    per_group = batch_rows // groups
    local_heads = KV_HEADS // PREFILL_TP
    head_share = HEADS // KV_HEADS
    layer_count = prefill_cache.shape[1]
    page_width = prefill_cache.shape[5]
    score_scale = (D / HEADS) ** (-0.5)
    q_cols = HEADS * HEAD_DIM
    k_cols = KV_HEADS * HEAD_DIM
    my_group = my_index // PREFILL_TP
    my_slot = my_index % PREFILL_TP
    group_rows = lax.dynamic_slice_in_dim(page_table, my_group * per_group, per_group, 0)
    group_lengths = lax.dynamic_slice_in_dim(lengths, my_group * per_group, per_group, 0)
    local_cache = prefill_cache[0]
    page_ids = jnp.arange(devices, dtype=jnp.int32)
    onehot = (group_rows[:, :, None] == page_ids[None, None, :]).astype(jnp.int32)
    inverse = jnp.sum(onehot * page_ids[None, :, None], axis=1)
    arranged = jax.vmap(take_pages, in_axes=(2, 0), out_axes=2)(local_cache, inverse)
    relaid = lax.all_to_all(arranged, "tp", split_axis=3, concat_axis=3, tiled=True)
    relaid = relaid.reshape(
        layer_count, 2, per_group, groups, PREFILL_TP, page_width, local_heads, HEAD_DIM
    )
    decode_local = relaid.transpose(0, 1, 3, 2, 5, 4, 6, 7).reshape(
        layer_count, 2, batch_rows, page_width, k_cols
    )
    my_pos = my_index * page_width + jnp.arange(page_width, dtype=jnp.int32)
    fresh_slot = my_pos[None, :] == lengths[:, None]
    kept_cache = local_cache.reshape(
        layer_count, 2, per_group, devices, page_width, local_heads, HEAD_DIM
    )
    cache_pos = (
        group_rows[:, :, None] * page_width + jnp.arange(page_width, dtype=jnp.int32)[None, None, :]
    )
    kept_visible = cache_pos < group_lengths[:, None, None]
    stream = hidden_in
    normed = rms_scale(stream, norm_gains[0, 0]).astype(jnp.bfloat16)
    column_part = project_rows(normed, qkv_weight[0]).astype(jnp.bfloat16)
    projected = lax.all_gather(column_part, "tp", axis=1, tiled=True)
    queries = rotate(
        projected[:, :q_cols].astype(jnp.float32).reshape(batch_rows, HEADS, HEAD_DIM), lengths
    ).astype(jnp.bfloat16)
    new_key = rotate(
        projected[:, q_cols : q_cols + k_cols]
        .astype(jnp.float32)
        .reshape(batch_rows, KV_HEADS, HEAD_DIM),
        lengths,
    ).astype(jnp.bfloat16)
    new_value = projected[:, q_cols + k_cols :]
    key_layer = jnp.where(
        fresh_slot[:, :, None], new_key.reshape(batch_rows, 1, k_cols), decode_local[0, 0]
    )
    value_layer = jnp.where(
        fresh_slot[:, :, None], new_value.reshape(batch_rows, 1, k_cols), decode_local[0, 1]
    )
    written = [jnp.stack([key_layer, value_layer], axis=0)]
    flat_q = queries.reshape(batch_rows, KV_HEADS, head_share, HEAD_DIM)
    flat_k = new_key.reshape(batch_rows, KV_HEADS, 1, HEAD_DIM)
    flat_v = new_value.reshape(batch_rows, KV_HEADS, 1, HEAD_DIM)
    own_weight = jnp.exp(
        capped(
            jnp.sum(flat_q.astype(jnp.float32) * flat_k.astype(jnp.float32), axis=-1) * score_scale
        )
    )
    own_term = round_back(own_weight)[..., None] * flat_v.astype(jnp.float32)
    shaped_q = flat_q.reshape(groups, per_group, PREFILL_TP, local_heads, head_share, HEAD_DIM)
    shaped_own = own_weight.reshape(groups, per_group, PREFILL_TP, local_heads, head_share)
    shaped_term = own_term.reshape(groups, per_group, PREFILL_TP, local_heads, head_share, HEAD_DIM)
    my_queries = pick_slot(shaped_q, my_group, my_slot)
    cached_keys = kept_cache[0, 0]
    cached_values = kept_cache[0, 1]
    raw_scores = (
        jnp.einsum("ramd,rjcad->ramjc", my_queries, cached_keys, preferred_element_type=jnp.float32)
        * score_scale
    )
    weights = jnp.where(kept_visible[:, None, None, :, :], jnp.exp(capped(raw_scores)), 0.0)
    numerator = jnp.einsum(
        "ramjc,rjcad->ramd",
        weights.astype(jnp.bfloat16),
        cached_values,
        preferred_element_type=jnp.float32,
    )
    numerator = numerator + pick_slot(shaped_term, my_group, my_slot)
    denominator = jnp.sum(weights, axis=(-2, -1)) + pick_slot(shaped_own, my_group, my_slot)
    mine = (
        (numerator / denominator[..., None])
        .astype(jnp.bfloat16)
        .reshape(1, per_group, local_heads * head_share * HEAD_DIM)
    )
    gathered = lax.all_gather(mine, "tp", axis=0, tiled=True)
    attended = (
        gathered.reshape(groups, PREFILL_TP, per_group, local_heads * head_share * HEAD_DIM)
        .transpose(0, 2, 1, 3)
        .reshape(batch_rows, q_cols)
    )
    mixed_part = project_rows(attended, out_weight[0]).astype(jnp.bfloat16)
    mixed_out = lax.all_gather(mixed_part, "tp", axis=1, tiled=True)
    stream = stream + rms_scale(mixed_out.astype(jnp.float32), norm_gains[0, 1])
    ffn_in = rms_scale(stream, norm_gains[0, 2]).astype(jnp.bfloat16)
    gate_proj = project_rows(ffn_in, gate_up_weight[0, 0])
    up_proj = project_rows(ffn_in, gate_up_weight[0, 1])
    active = (jax.nn.gelu(gate_proj, approximate=True) * up_proj).astype(jnp.bfloat16)
    branch = jnp.dot(active, down_weight[0], preferred_element_type=jnp.float32)
    column_count = branch.shape[1] // devices
    summed = lax.psum(branch, "tp")
    stream = stream + rms_scale(summed, norm_gains[0, 3])
    result = lax.dynamic_slice_in_dim(stream, my_index * column_count, column_count, 1)
    decode_cache = jnp.stack(written, axis=0)[None]
    return (result, decode_cache)


MESH = pl.DeviceIdType.MESH
LANES = 128
NT = (((1,), (1,)), ((), ()))
LOG_BASE = 9.210340371976184
UNROLL = True
VMEM_LIMIT = 58 * 1024 * 1024


def dot_t(left, right):
    return lax.dot_general(left, right, NT, preferred_element_type=jnp.float32)


def normed_by(vector, meansq, gain):
    return vector * lax.rsqrt(meansq + EPSILON) * (1.0 + gain)


def meansq_of(vector):
    return jnp.mean(vector * vector, axis=-1, keepdims=True)


def column_of(scalars, count):
    row = lax.broadcasted_iota(jnp.int32, (count, 1), 0)
    column = jnp.zeros((count, 1), jnp.int32)
    for i in range(count):
        column = jnp.where(row == i, scalars[i], column)
    return column.astype(jnp.float32)


def pad_rows(rows, count):
    return jnp.concatenate(
        [rows, jnp.zeros((count - rows.shape[0], rows.shape[1]), rows.dtype)], axis=0
    )


def fused_kernel(
    dims,
    len_hbm,
    table_hbm,
    hid_hbm,
    gain_hbm,
    flat_hbm,
    wq_hbm,
    wo_hbm,
    wgu_hbm,
    wd_hbm,
    out_ref,
    dec_done,
    len_ref,
    hid,
    gain,
    table,
    flat,
    wq,
    wo,
    wgu,
    wd,
    proj,
    att,
    attended,
    mix,
    branch,
    arrive,
    sums,
    squares,
    stack,
    mixed_ref,
    blend,
    page_stage,
    dec,
    load_sem,
    send_sem,
    proj_sem,
    att_sem,
    mix_sem,
    tail_sem,
):
    T, B, R, RP = dims["T"], dims["B"], dims["R"], dims["RP"]
    share, local_heads, slots = dims["share"], dims["local_heads"], dims["S"]
    per_group, groups = dims["per_group"], dims["groups"]
    planes, plane_size = dims["planes"], dims["plane_size"]
    first_owner, owner_count = dims["first_owner"], dims["owner_count"]
    width = local_heads * HEAD_DIM
    cols = wq.shape[0]
    heads_here = cols // HEAD_DIM
    q_devs = HEADS * HEAD_DIM // cols
    k_devs = KV_HEADS * HEAD_DIM // cols
    page_width = dec.shape[2]
    model = wq.shape[1]
    ff = wd.shape[0]
    chunks = model // LANES
    score_scale = (D / HEADS) ** (-0.5)
    me = lax.axis_index("tp")
    my_group = me // PREFILL_TP
    my_slot = me % PREFILL_TP
    my_plane = me // plane_size
    my_seat = me % plane_size

    def load(index, src, dst):
        return pltpu.make_async_copy(src, dst, load_sem.at[index])

    small = [
        load(0, hid_hbm, hid.at[:, pl.ds(0, model)]),
        load(1, gain_hbm, gain.at[:, pl.ds(0, model)]),
        load(2, len_hbm, len_ref),
        load(3, table_hbm, table),
    ]
    cuts = dims["cuts"]
    wq_loads = [
        load(8 + i, wq_hbm.at[:, pl.ds(lo, hi - lo)], wq.at[:, pl.ds(lo, hi - lo)])
        for i, (lo, hi) in enumerate(cuts)
    ]
    flat_load = load(4, flat_hbm, flat)
    wo_load = load(5, wo_hbm, wo)
    wgu_load = load(6, wgu_hbm, wgu)
    wd_load = load(7, wd_hbm, wd)
    for piece in small + wq_loads + [flat_load, wo_load, wgu_load, wd_load]:
        piece.start()

    barrier = pltpu.get_barrier_semaphore()

    for step in range(1, T):
        peer = lax.rem(me + step, T)
        pl.semaphore_signal(barrier, inc=1, device_id={"tp": peer}, device_id_type=MESH)

    def dec_part(ref, index):
        group, slot = index // PREFILL_TP, index % PREFILL_TP
        lane = pl.multiple_of(slot * width, width)
        return ref.at[:, pl.ds(group * per_group, per_group), :, pl.ds(lane, width)]

    def remote(src, dst, send, recv, peer):
        return pltpu.make_async_remote_copy(
            src_ref=src,
            dst_ref=dst,
            send_sem=send_sem.at[send],
            recv_sem=recv,
            device_id={"tp": peer},
            device_id_type=MESH,
        )

    def sent(send, ref):
        remote(ref, ref, send, tail_sem.at[0], me).wait_send()

    def landed(recv, ref):
        remote(ref, ref, 0, recv, me).wait_recv()

    def owners(index):
        first = index % PREFILL_TP * local_heads
        key = first // heads_here
        return (first * share // heads_here, q_devs + key, q_devs + k_devs + key)

    def proj_from(sender):
        return proj_sem.at[jnp.maximum(sender - (q_devs - 1), 0)]

    def send_proj(peer):
        remote(proj.at[me], proj.at[me], 0, proj_from(me), peer).start()

    def send_urgent():
        @pl.when(me < q_devs)
        def _():
            send_proj(me + PREFILL_TP)

        @pl.when(me >= q_devs)
        def _():
            first = (me - q_devs) % k_devs * (PREFILL_TP // k_devs)
            for g in range(groups):
                for i in range(PREFILL_TP // k_devs):
                    peer = g * PREFILL_TP + first + i
                    if g == 0:
                        send_proj(peer)
                        continue

                    @pl.when(peer != me)
                    def _():
                        send_proj(peer)

    def send_others():
        for step in range(1, T):
            peer = lax.rem(me + step, T)
            q_owner, k_owner, v_owner = owners(peer)

            @pl.when((k_owner != me) & (v_owner != me) & (me >= q_devs))
            def _():
                send_proj(peer)

    def take_proj(sender):
        @pl.when(sender != me)
        def _():
            landed(proj_from(sender), proj.at[sender])

    def push_pages(begin, end):
        for step in range(begin, min(end, T)):
            peer = lax.rem(me + step, T)
            remote(page_stage.at[peer], dec_part(dec, me), 1, tail_sem.at[3], peer).start()

    def push(send, recv, src, near_first=False):
        upper = my_plane // (planes // 2)
        for turn_of in range(planes):
            if near_first:
                plane = jnp.where(upper == 0, turn_of, planes - 1 - turn_of)
            else:
                plane = jnp.where(upper == 0, planes - 1 - turn_of, turn_of)
            for seat in range(plane_size):
                peer = plane * plane_size + lax.rem(my_seat + seat, plane_size)
                if seat:
                    remote(src, src, send, recv, peer).start()
                    continue

                @pl.when(plane != my_plane)
                def _():
                    remote(src, src, send, recv, peer).start()

    def take_plane(sems, ref, plane):
        first = plane * plane_size

        @pl.when(plane == my_plane)
        def _():
            landed(sems.at[plane], ref.at[pl.ds(first, plane_size - 1)])

        @pl.when(plane != my_plane)
        def _():
            landed(sems.at[plane], ref.at[pl.ds(first, plane_size)])

    small[2].wait()
    length = column_of(len_ref, B)
    lane = lax.broadcasted_iota(jnp.int32, (B, HEAD_DIM), 1)
    half = HEAD_DIM // 2
    exponent = (lane % half).astype(jnp.float32) * (-2.0 / HEAD_DIM)
    angles = length * jnp.exp(exponent * LOG_BASE)
    turning = jnp.broadcast_to(me < q_devs + k_devs, lane.shape)
    cosine = jnp.where(turning, jnp.cos(angles), 1.0)
    sine = jnp.where(turning, jnp.where(lane < half, -1.0, 1.0) * jnp.sin(angles), 0.0)
    small[3].wait()
    slot_page = lax.broadcasted_iota(jnp.int32, (T, slots), 1) // page_width
    spread = (slot_page == lax.broadcasted_iota(jnp.int32, (T, slots), 0)).astype(jnp.float32)
    inside = lax.broadcasted_iota(jnp.int32, (B, slots), 1) % page_width
    position = jnp.dot(
        table[...].astype(jnp.float32).astype(jnp.bfloat16),
        spread.astype(jnp.bfloat16),
        preferred_element_type=jnp.float32,
    ) * page_width + inside.astype(jnp.float32)
    request_of = lax.broadcasted_iota(jnp.int32, (B, slots), 0)

    def row_at(values, request):
        return jnp.sum(jnp.where(request_of == request, values, 0.0), axis=0, keepdims=True)

    place = [row_at(position, my_group * per_group + e) for e in range(per_group)]
    limit = [
        row_at(jnp.broadcast_to(length, (B, slots)), my_group * per_group + e)
        for e in range(per_group)
    ]
    small[0].wait()
    small[1].wait()
    stream = hid[:, :model]
    normed = normed_by(stream, meansq_of(stream), gain[0:1, :model]).astype(jnp.bfloat16)
    part = jnp.zeros((B, cols), jnp.float32)
    for (lo, hi), piece in zip(cuts, wq_loads):
        piece.wait()
        part = part + dot_t(normed[:, lo:hi], wq[:, lo:hi])
    part = part.astype(jnp.bfloat16).astype(jnp.float32)
    for head in range(heads_here):
        u = part[:, head * HEAD_DIM : (head + 1) * HEAD_DIM]
        swapped = jnp.concatenate([u[:, half:], u[:, :half]], axis=1)
        turned = u * cosine + swapped * sine
        proj[me, :, head * HEAD_DIM : (head + 1) * HEAD_DIM] = turned.astype(jnp.bfloat16)
    pl.semaphore_wait(barrier, T - 1)
    send_urgent()

    flat_load.wait()
    wanted = lax.broadcasted_iota(jnp.int32, (slots, slots), 0).astype(jnp.float32)
    for e in range(per_group):
        pick = (wanted == place[e]).astype(jnp.float32).astype(jnp.bfloat16)
        for c in range(2):
            moved = jnp.dot(pick, flat[c, e], preferred_element_type=jnp.float32)
            page_stage[:, c, e] = moved.reshape(T, page_width, width).astype(jnp.bfloat16)
    push_pages(1, dims["page_cut"])
    q_from, k_from, v_from = owners(me)
    take_proj(q_from)
    take_proj(k_from)

    rows = share * B
    row_of = lax.broadcasted_iota(jnp.int32, (rows, HEAD_DIM), 0)

    def head_of(owner, index):
        at = pl.multiple_of((index % heads_here) * HEAD_DIM, HEAD_DIM)
        return proj[owner, :, pl.ds(at, HEAD_DIM)].astype(jnp.float32)

    found = {}
    for a in range(local_heads):
        kv_head = my_slot * local_heads + a
        q = jnp.concatenate([head_of(q_from, kv_head * share + m) for m in range(share)], axis=0)
        k_new = jnp.concatenate([head_of(k_from, kv_head)] * share, axis=0)
        q16 = q.astype(jnp.bfloat16)
        own = jnp.exp(capped(jnp.sum(q * k_new, axis=-1, keepdims=True) * score_scale))
        lanes = slice(a * HEAD_DIM, (a + 1) * HEAD_DIM)
        for e in range(per_group):
            scores = dot_t(q16, flat[0, e, :, lanes]) * score_scale
            weights = jnp.where(place[e] < limit[e], jnp.exp(capped(scores)), 0.0)
            numer = jnp.dot(
                weights.astype(jnp.bfloat16),
                flat[1, e, :, lanes],
                preferred_element_type=jnp.float32,
            )
            found[a, e] = (numer, jnp.sum(weights, axis=-1, keepdims=True) + own, own)
    take_proj(v_from)
    for a in range(local_heads):
        kv_head = my_slot * local_heads + a
        v_new = jnp.concatenate([head_of(v_from, kv_head)] * share, axis=0)
        picked = [[] for m in range(share)]
        for e in range(per_group):
            request = my_group * per_group + e
            numer, denom, own = found[a, e]
            result = (numer + own.astype(jnp.bfloat16).astype(jnp.float32) * v_new) / denom
            for m in range(share):
                chosen = jnp.where(row_of == m * B + request, result, 0.0)
                picked[m].append(jnp.sum(chosen, axis=0, keepdims=True))
        for m in range(share):
            at = (a * share + m) * HEAD_DIM
            att[me, :, at : at + HEAD_DIM] = jnp.concatenate(picked[m], axis=0).astype(jnp.bfloat16)
    push(2, att_sem.at[my_plane], att.at[me])
    send_others()

    first_lane = pl.multiple_of(me * R // LANES * LANES, LANES)
    window = RP + LANES
    turn = window - lax.rem(me * R, LANES)
    own_hid = pltpu.roll(hid[:, pl.ds(first_lane, window)], turn, 1)[:, :RP]
    own_gain = pltpu.roll(gain[:, pl.ds(first_lane, window)], turn, 1)[:, :RP]
    wo_load.wait()
    q_width = att.shape[2]
    halves = T // PREFILL_TP
    slots_half = PREFILL_TP // halves
    half_width = slots_half * q_width
    for p in range(planes):
        take_plane(att_sem, att, jnp.int32(p))
    pieces = [
        jnp.concatenate(
            [att[g * PREFILL_TP + s].astype(jnp.float32) for g in range(groups)], axis=0
        )
        for s in range(PREFILL_TP)
    ]
    probe = pad_rows(jnp.concatenate(pieces, axis=1).astype(jnp.bfloat16), SUBLANES)
    pair = R // 2
    pair_lane = pair // LANES * LANES
    both = dot_t(
        jnp.concatenate([probe, wo[pair:, :]], axis=0),
        jnp.concatenate([wo[:pair, :], probe], axis=0),
    )
    rest = both[SUBLANES:, pair_lane:]
    rest = jnp.concatenate([rest, jnp.zeros((pair, LANES - rest.shape[1]), jnp.float32)], axis=1).T
    mixed = jnp.concatenate([both[:B, :pair], rest[pair - pair_lane : pair - pair_lane + B]], axis=1)
    mixed = mixed.astype(jnp.bfloat16).astype(jnp.float32)
    mixed = jnp.concatenate([mixed, jnp.zeros((B, RP - R), jnp.float32)], axis=1)
    shift = dims["seat_shift"]
    mix[me] = pltpu.roll(mixed, my_seat * shift, 1).astype(jnp.bfloat16)
    push(3, mix_sem.at[my_plane], mix.at[me], True)
    blend[:B, :] = hid[:, :model] * (1.0 + gain[2:3, :model])
    wgu_load.wait()
    side = ff // 2
    tile = dims["ff_tile"]
    at_lane = tile // LANES * LANES
    blocks = [(s, c) for s in range(side // tile) for c in range(2)]
    half_cols = model // halves
    half_seats = T // halves
    front, upright = {}, {}
    for turn_of in range(halves):
        which = (my_plane // (planes // halves) + turn_of) % halves
        for p in range(planes // halves):
            plane = which * (planes // halves) + p
            if turn_of:
                landed(mix_sem.at[plane], mix.at[pl.ds(plane * plane_size, plane_size)])
            else:
                take_plane(mix_sem, mix, plane)
        if turn_of == 0:
            push_pages(dims["page_cut"], T)
        tiles = [None] * (half_cols // LANES)
        for s in range(half_seats):
            block = mix[which * half_seats + s].astype(jnp.float32)
            for i in range(RP // LANES):
                at = s * R // LANES + i
                piece = block[:, i * LANES : (i + 1) * LANES]
                if at < len(tiles):
                    tiles[at] = piece if tiles[at] is None else tiles[at] + piece
        got = jnp.concatenate(tiles, axis=1)
        span_at = pl.ds(pl.multiple_of(which * half_cols, LANES), half_cols)
        mixed_ref[:, span_at] = got
        blend[B:, span_at] = got * ((1.0 + gain[1:2, span_at]) * (1.0 + gain[2:3, span_at]))
        exact = blend[:, span_at]
        high = exact.astype(jnp.bfloat16).astype(jnp.float32)
        probe = jnp.concatenate([high, exact - high], axis=0).astype(jnp.bfloat16)
        if turn_of == halves - 1:
            mixed_all = mixed_ref[...]
            mixed_ms = meansq_of(mixed_all)
            stream = hid[:, :model] + normed_by(mixed_all, mixed_ms, gain[1:2, :model])
            outer = lax.rsqrt(meansq_of(stream) + EPSILON)
            inner = lax.rsqrt(mixed_ms + EPSILON)
            mine = own_hid + normed_by(mixed, mixed_ms, own_gain[1:2, :])
        for s, c in blocks:
            at = s * tile
            pushed = jnp.concatenate([wgu[c, at : at + tile, span_at], probe], axis=0)
            passed = jnp.concatenate(
                [probe, wgu[c, side + at : side + at + tile, span_at]], axis=0
            )
            both = dot_t(passed, pushed)
            part = both[: 2 * B, :tile] + both[2 * B : 4 * B, :tile]
            front[s, c] = part if turn_of == 0 else front[s, c] + part
            rest = both[4 * B :, at_lane:]
            wide = rest.shape[1]
            if turn_of < halves - 1:
                stack[s, c, :, :wide] = rest
            else:
                rest = jnp.concatenate(
                    [rest + stack[s, c, :, :wide], jnp.zeros((tile, LANES - wide), jnp.float32)],
                    axis=1,
                )
                turned = rest.T
                first = tile - at_lane
                upright[s, c] = turned[first : first + 2 * B] + turned[first + 2 * B : first + 4 * B]

    def settle(parts):
        return outer * (parts[:B] + inner * parts[B:])

    steps = range(side // tile)
    active = []
    for table_of in (front, upright):
        for s in steps:
            gate, up = settle(table_of[s, 0]), settle(table_of[s, 1])
            active.append(jax.nn.gelu(gate, approximate=True) * up)
    active = jnp.concatenate(active, axis=1).astype(jnp.bfloat16)
    wd_load.wait()
    owned = model // owner_count
    span = arrive.shape[2]
    is_owner = (me >= first_owner) & (me < first_owner + owner_count)
    side_owners = owner_count // halves
    for turn_of in range(halves):
        which = (halves - 1 - my_plane // (planes // halves) + turn_of) % halves
        half_at = pl.multiple_of(which * half_cols, LANES)
        wide = -(-half_cols // (4 * LANES)) * 4 * LANES
        done_cols = wide if turn_of == 0 else model - wide
        done_at = pl.multiple_of(which * (model - done_cols), LANES)
        part = jnp.dot(active, wd[:, pl.ds(done_at, done_cols)], preferred_element_type=jnp.float32)
        branch[:, pl.ds(done_at, done_cols)] = part.astype(jnp.bfloat16)
        for i in range(side_owners):
            peer = first_owner + which * side_owners + i

            @pl.when(me != peer)
            def _():
                begin = pl.multiple_of(half_at + i * owned // LANES * LANES, LANES)
                remote(branch.at[:, pl.ds(begin, span)], arrive.at[me], 4, tail_sem.at[0], peer).start()

    @pl.when(is_owner)
    def _():
        o = me - first_owner
        odd = o % 2
        base = pl.multiple_of(o * owned // LANES * LANES, LANES)
        total = branch[:, pl.ds(base, span)].astype(jnp.float32)
        landed(tail_sem.at[0], arrive.at[pl.ds(0, T - 1)])
        for s in range(T):
            piece = arrive[s].astype(jnp.float32)
            total = total + jnp.where(me == s, 0.0, piece)
        offset = odd * (LANES // 2)
        lane_of = lax.broadcasted_iota(jnp.int32, (B, span), 1)
        inside = (lane_of >= offset) & (lane_of < offset + owned)
        kept = jnp.where(inside, total, 0.0)
        ready = []
        for i in range(2):
            begin = i * R // LANES * LANES
            left = RP - (i * R - begin) - offset
            ready.append(pltpu.roll(kept[:, begin : begin + RP], lax.rem(left, RP), 1))
            sums[i] = ready[i]
        for i in range(2):
            peer = o * 2 + i

            @pl.when(peer != me)
            def _():
                remote(sums.at[i], sums.at[2], 5, tail_sem.at[1], peer).start()

            @pl.when(peer == me)
            def _():
                sums[2] = ready[i]

        each = jnp.sum(kept * kept, axis=-1, keepdims=True)
        spot = lax.broadcasted_iota(jnp.int32, (B, LANES), 1) == lax.broadcasted_iota(
            jnp.int32, (B, LANES), 0
        )
        squares[o] = jnp.sum(jnp.where(spot, each, 0.0), axis=0, keepdims=True)
        push(6, tail_sem.at[2], squares.at[o])

    dec_part(dec, me)[...] = page_stage[me]
    landed(tail_sem.at[3], page_stage.at[pl.ds(0, T - 1)])
    for owner in range(q_devs, q_devs + 2 * k_devs):
        @pl.when((owner != k_from) & (owner != v_from))
        def _():
            take_proj(jnp.int32(owner))

    token = lax.broadcasted_iota(jnp.int32, (page_width, cols), 0) + me * page_width
    for c in range(2):
        for i in range(k_devs):
            fresh = proj[q_devs + c * k_devs + i].astype(jnp.float32)
            for r in range(B):
                old = dec[c, r, :, i * cols : (i + 1) * cols].astype(jnp.float32)
                row = jnp.broadcast_to(fresh[r : r + 1, :], old.shape)
                new = jnp.where(token == len_ref[r], row, old)
                dec_done[c, r, :, i * cols : (i + 1) * cols] = new.astype(jnp.bfloat16)

    for send, ref in ((2, att), (3, mix)):
        sent(send, ref.at[pl.ds(0, T - 1)])
    sent(1, page_stage.at[pl.ds(0, T - 1)])

    @pl.when(me < q_devs)
    def _():
        sent(0, proj.at[0])

    @pl.when(me >= q_devs)
    def _():
        sent(0, proj.at[pl.ds(0, T - 1)])

    @pl.when(is_owner)
    def _():
        sent(4, arrive.at[pl.ds(0, owner_count - 1)])
        landed(tail_sem.at[2], squares.at[pl.ds(0, owner_count - 1)])

    @pl.when(jnp.logical_not(is_owner))
    def _():
        sent(4, arrive.at[pl.ds(0, owner_count)])
        landed(tail_sem.at[2], squares.at[pl.ds(0, owner_count)])

    @pl.when(first_owner + me // 2 != me)
    def _():
        landed(tail_sem.at[1], sums.at[2])

    sumsq = squares[0]
    for s in range(1, owner_count):
        sumsq = sumsq + squares[s]
    spot = lax.broadcasted_iota(jnp.int32, (B, LANES), 1) == lax.broadcasted_iota(
        jnp.int32, (B, LANES), 0
    )
    branch_ms = jnp.sum(
        jnp.where(spot, jnp.broadcast_to(sumsq, (B, LANES)), 0.0), axis=-1, keepdims=True
    ) * (1.0 / model)
    result = mine + normed_by(sums[2], branch_ms, own_gain[3:4, :])
    out_ref[...] = result[:, :R]

    @pl.when(is_owner)
    def _():
        o = me - first_owner
        sent(6, arrive_like(squares, T - 1, owner_count))

        @pl.when(o * 2 == me)
        def _():
            sent(5, sums.at[0])

        @pl.when(o * 2 + 1 == me)
        def _():
            sent(5, sums.at[0])

        @pl.when((o * 2 != me) & (o * 2 + 1 != me))
        def _():
            sent(5, sums.at[pl.ds(0, 2)])


def arrive_like(squares, count, limit):
    return squares.at[pl.ds(0, count)]


def finish_kernel(out_ref, dec_ref, out_hbm, dec_hbm, sem):
    first = pltpu.make_async_copy(dec_ref, dec_hbm, sem.at[0])
    second = pltpu.make_async_copy(out_ref, out_hbm, sem.at[1])
    first.start()
    second.start()
    first.wait()
    second.wait()


def fits_kernel(shapes, devices):
    batch_rows, model = shapes["hidden"]
    cols, rows, ff = shapes["qkv"], shapes["out"], shapes["ff"]
    groups = devices // PREFILL_TP
    weight_bytes = 2 * (cols * model + rows * HEADS * HEAD_DIM + 3 * ff * model)
    return (
        devices == 2 * PREFILL_TP
        and cols == HEADS // PREFILL_TP * HEAD_DIM
        and (KV_HEADS * HEAD_DIM) % cols == 0
        and (HEADS * HEAD_DIM) % cols == 0
        and batch_rows % groups == 0
        and model % (LANES * 2) == 0
        and ff % (6 * SUBLANES) == 0
        and rows * devices == model
        and rows * 4 % LANES == 0
        and rows % (2 * SUBLANES) == 0
        and weight_bytes < VMEM_LIMIT * 3 // 4
        and batch_rows == 4
    )


SUBLANES = 16


def fused_device(
    hidden_in,
    prefill_cache,
    lengths,
    page_table,
    qkv_weight,
    out_weight,
    gate_up_weight,
    down_weight,
    norm_gains,
):
    T = lax.axis_size("tp")
    B, model = hidden_in.shape
    groups = T // PREFILL_TP
    per_group = B // groups
    local_heads = KV_HEADS // PREFILL_TP
    share = HEADS // KV_HEADS
    pages, page_width, width = prefill_cache.shape[4:]
    S = pages * page_width
    cols = qkv_weight.shape[1]
    R = out_weight.shape[1]
    RP = -(-R // LANES) * LANES
    ff = down_weight.shape[1]
    k_cols = KV_HEADS * HEAD_DIM
    planes = 4
    plane_size = T // planes
    owner_count = T // 2
    depth = model // 256
    marks = list(range(0, depth, 2)) + [depth]
    dims = dict(
        T=T, B=B, R=R, RP=RP, S=S, share=share, local_heads=local_heads,
        per_group=per_group, groups=groups, planes=planes, plane_size=plane_size,
        first_owner=plane_size, owner_count=owner_count, seat_shift=R % LANES,
        cuts=[(lo * 256, hi * 256) for lo, hi in zip(marks, marks[1:])],
        ff_tile=ff // 6, page_cut=T // 2,
    )
    q_width = local_heads * share * HEAD_DIM
    span = -(-(model // owner_count) // LANES) * LANES
    bf16, f32 = jnp.bfloat16, jnp.float32
    vmem = pl.BlockSpec(memory_space=pltpu.VMEM)
    anyw = pl.BlockSpec(memory_space=pl.ANY)
    out, dec = pl.pallas_call(
        functools.partial(fused_kernel, dims),
        out_shape=(
            pltpu.VMEM((B, R), f32),
            pltpu.VMEM((2, B, page_width, k_cols), bf16),
        ),
        in_specs=[anyw] * 9,
        out_specs=(vmem, vmem),
        scratch_shapes=[
            pltpu.SMEM((B,), jnp.int32),
            pltpu.VMEM((B, model + RP), f32),
            pltpu.VMEM((norm_gains.shape[1], model + RP), f32),
            pltpu.VMEM((B, T), jnp.int32),
            pltpu.VMEM((2, per_group, S, width), bf16),
            pltpu.VMEM((cols, model), bf16),
            pltpu.VMEM((R, HEADS * HEAD_DIM), bf16),
            pltpu.VMEM((2, ff, model), bf16),
            pltpu.VMEM((ff, model), bf16),
            pltpu.VMEM((T, B, cols), bf16),
            pltpu.VMEM((T, per_group, q_width), bf16),
            pltpu.VMEM((B, HEADS * HEAD_DIM), bf16),
            pltpu.VMEM((T, B, RP), bf16),
            pltpu.VMEM((B, model), bf16),
            pltpu.VMEM((T, B, span), bf16),
            pltpu.VMEM((3, B, RP), f32),
            pltpu.VMEM((T, 1, LANES), f32),
            pltpu.VMEM((3, 2, ff // 6, LANES), f32),
            pltpu.VMEM((B, model), f32),
            pltpu.VMEM((2 * B, model), f32),
            pltpu.VMEM((T, 2, per_group, page_width, width), bf16),
            pltpu.VMEM((2, B, page_width, k_cols), bf16),
            pltpu.SemaphoreType.DMA((8 + len(dims["cuts"]),)),
            pltpu.SemaphoreType.DMA((7,)),
            pltpu.SemaphoreType.DMA((9,)),
            pltpu.SemaphoreType.DMA((4,)),
            pltpu.SemaphoreType.DMA((4,)),
            pltpu.SemaphoreType.DMA((4,)),
        ],
        compiler_params=pltpu.CompilerParams(
            collective_id=0, has_side_effects=True, vmem_limit_bytes=VMEM_LIMIT
        ),
    )(
        lengths,
        page_table,
        hidden_in,
        norm_gains[0],
        prefill_cache.reshape(2, per_group, S, width),
        qkv_weight[0],
        out_weight[0],
        gate_up_weight[0],
        down_weight[0],
    )
    out, dec = pl.pallas_call(
        finish_kernel,
        out_shape=(
            jax.ShapeDtypeStruct((B, R), f32),
            jax.ShapeDtypeStruct((2, B, page_width, k_cols), bf16),
        ),
        in_specs=[vmem, vmem],
        out_specs=(anyw, anyw),
        scratch_shapes=[pltpu.SemaphoreType.DMA((2,))],
    )(
        pltpu.with_memory_space_constraint(out, pltpu.VMEM),
        pltpu.with_memory_space_constraint(dec, pltpu.VMEM),
    )
    return out, dec.reshape(1, 1, 2, B, page_width, k_cols)


def step(*args):
    shapes = {
        "hidden": args[0].shape,
        "qkv": args[4].shape[1],
        "out": args[5].shape[1],
        "ff": args[7].shape[1],
    }
    chosen = fused_device if fits_kernel(shapes, lax.axis_size("tp")) else on_device
    return chosen(*args)


def solution(mesh):
    placed = (
        P("grp", None),
        P("tp", None, None, "grp", None, None, None),
        P("grp"),
        P("grp", None),
        P(None, "tp", None),
        P(None, "tp", None),
        P(None, None, "tp", None),
        P(None, "tp", None),
        P(),
    )
    return jax.shard_map(
        step,
        mesh=mesh,
        in_specs=placed,
        out_specs=(P("grp", "tp"), P("tp", None, None, "grp", None, None)),
        check_vma=False,
    )
```

```python
import functools

import jax
import jax.numpy as jnp
from jax import lax
from jax.experimental import pallas as pl
from jax.experimental.pallas import tpu as pltpu
from jax.sharding import PartitionSpec as P

D = 4608
HEADS = 32
KV_HEADS = 16
HEAD_DIM = 128
PREFILL_TP = 8


EPSILON = 1e-06
SOFTCAP = 50.0


def rms_scale(vector, gain_row):
    meansq = jnp.mean(vector * vector, axis=-1, keepdims=True)
    return vector * lax.rsqrt(meansq + EPSILON) * (1.0 + gain_row)


def rotate(vector, positions):
    half_dim = vector.shape[-1] // 2
    exponent = jnp.arange(half_dim, dtype=jnp.float32) * (-2.0 / vector.shape[-1])
    frequency = jnp.power(jnp.float32(10000.0), exponent)
    angles = positions.astype(jnp.float32)[:, None, None] * frequency
    cosine = jnp.cos(angles)
    sine_term = jnp.sin(angles)
    front_half = vector[..., :half_dim]
    back_half = vector[..., half_dim:]
    return jnp.concatenate(
        [front_half * cosine - back_half * sine_term, back_half * cosine + front_half * sine_term],
        axis=-1,
    )


def capped(raw_scores):
    return SOFTCAP * jnp.tanh(raw_scores / SOFTCAP)


def round_back(vector):
    return lax.optimization_barrier(vector.astype(jnp.bfloat16)).astype(jnp.float32)


def pick_slot(vector, my_group, my_slot):
    inner = lax.dynamic_index_in_dim(vector, my_group, 0, False)
    return lax.dynamic_index_in_dim(inner, my_slot, 1, False)


def take_pages(page_block, page_order):
    return jnp.take(page_block, page_order, axis=2)


def project_rows(left, weight_rows):
    return jnp.einsum("bd,cd->bc", left, weight_rows, preferred_element_type=jnp.float32)


def on_device(
    hidden_in,
    prefill_cache,
    lengths,
    page_table,
    qkv_weight,
    out_weight,
    gate_up_weight,
    down_weight,
    norm_gains,
):
    devices = lax.axis_size("tp")
    my_index = lax.axis_index("tp")
    batch_rows = hidden_in.shape[0]
    groups = devices // PREFILL_TP
    per_group = batch_rows // groups
    local_heads = KV_HEADS // PREFILL_TP
    head_share = HEADS // KV_HEADS
    layer_count = prefill_cache.shape[1]
    page_width = prefill_cache.shape[5]
    score_scale = (D / HEADS) ** (-0.5)
    q_cols = HEADS * HEAD_DIM
    k_cols = KV_HEADS * HEAD_DIM
    my_group = my_index // PREFILL_TP
    my_slot = my_index % PREFILL_TP
    group_rows = lax.dynamic_slice_in_dim(page_table, my_group * per_group, per_group, 0)
    group_lengths = lax.dynamic_slice_in_dim(lengths, my_group * per_group, per_group, 0)
    local_cache = prefill_cache[0]
    page_ids = jnp.arange(devices, dtype=jnp.int32)
    onehot = (group_rows[:, :, None] == page_ids[None, None, :]).astype(jnp.int32)
    inverse = jnp.sum(onehot * page_ids[None, :, None], axis=1)
    arranged = jax.vmap(take_pages, in_axes=(2, 0), out_axes=2)(local_cache, inverse)
    relaid = lax.all_to_all(arranged, "tp", split_axis=3, concat_axis=3, tiled=True)
    relaid = relaid.reshape(
        layer_count, 2, per_group, groups, PREFILL_TP, page_width, local_heads, HEAD_DIM
    )
    decode_local = relaid.transpose(0, 1, 3, 2, 5, 4, 6, 7).reshape(
        layer_count, 2, batch_rows, page_width, k_cols
    )
    my_pos = my_index * page_width + jnp.arange(page_width, dtype=jnp.int32)
    fresh_slot = my_pos[None, :] == lengths[:, None]
    kept_cache = local_cache.reshape(
        layer_count, 2, per_group, devices, page_width, local_heads, HEAD_DIM
    )
    cache_pos = (
        group_rows[:, :, None] * page_width + jnp.arange(page_width, dtype=jnp.int32)[None, None, :]
    )
    kept_visible = cache_pos < group_lengths[:, None, None]
    stream = hidden_in
    normed = rms_scale(stream, norm_gains[0, 0]).astype(jnp.bfloat16)
    column_part = project_rows(normed, qkv_weight[0]).astype(jnp.bfloat16)
    projected = lax.all_gather(column_part, "tp", axis=1, tiled=True)
    queries = rotate(
        projected[:, :q_cols].astype(jnp.float32).reshape(batch_rows, HEADS, HEAD_DIM), lengths
    ).astype(jnp.bfloat16)
    new_key = rotate(
        projected[:, q_cols : q_cols + k_cols]
        .astype(jnp.float32)
        .reshape(batch_rows, KV_HEADS, HEAD_DIM),
        lengths,
    ).astype(jnp.bfloat16)
    new_value = projected[:, q_cols + k_cols :]
    key_layer = jnp.where(
        fresh_slot[:, :, None], new_key.reshape(batch_rows, 1, k_cols), decode_local[0, 0]
    )
    value_layer = jnp.where(
        fresh_slot[:, :, None], new_value.reshape(batch_rows, 1, k_cols), decode_local[0, 1]
    )
    written = [jnp.stack([key_layer, value_layer], axis=0)]
    flat_q = queries.reshape(batch_rows, KV_HEADS, head_share, HEAD_DIM)
    flat_k = new_key.reshape(batch_rows, KV_HEADS, 1, HEAD_DIM)
    flat_v = new_value.reshape(batch_rows, KV_HEADS, 1, HEAD_DIM)
    own_weight = jnp.exp(
        capped(
            jnp.sum(flat_q.astype(jnp.float32) * flat_k.astype(jnp.float32), axis=-1) * score_scale
        )
    )
    own_term = round_back(own_weight)[..., None] * flat_v.astype(jnp.float32)
    shaped_q = flat_q.reshape(groups, per_group, PREFILL_TP, local_heads, head_share, HEAD_DIM)
    shaped_own = own_weight.reshape(groups, per_group, PREFILL_TP, local_heads, head_share)
    shaped_term = own_term.reshape(groups, per_group, PREFILL_TP, local_heads, head_share, HEAD_DIM)
    my_queries = pick_slot(shaped_q, my_group, my_slot)
    cached_keys = kept_cache[0, 0]
    cached_values = kept_cache[0, 1]
    raw_scores = (
        jnp.einsum("ramd,rjcad->ramjc", my_queries, cached_keys, preferred_element_type=jnp.float32)
        * score_scale
    )
    weights = jnp.where(kept_visible[:, None, None, :, :], jnp.exp(capped(raw_scores)), 0.0)
    numerator = jnp.einsum(
        "ramjc,rjcad->ramd",
        weights.astype(jnp.bfloat16),
        cached_values,
        preferred_element_type=jnp.float32,
    )
    numerator = numerator + pick_slot(shaped_term, my_group, my_slot)
    denominator = jnp.sum(weights, axis=(-2, -1)) + pick_slot(shaped_own, my_group, my_slot)
    mine = (
        (numerator / denominator[..., None])
        .astype(jnp.bfloat16)
        .reshape(1, per_group, local_heads * head_share * HEAD_DIM)
    )
    gathered = lax.all_gather(mine, "tp", axis=0, tiled=True)
    attended = (
        gathered.reshape(groups, PREFILL_TP, per_group, local_heads * head_share * HEAD_DIM)
        .transpose(0, 2, 1, 3)
        .reshape(batch_rows, q_cols)
    )
    mixed_part = project_rows(attended, out_weight[0]).astype(jnp.bfloat16)
    mixed_out = lax.all_gather(mixed_part, "tp", axis=1, tiled=True)
    stream = stream + rms_scale(mixed_out.astype(jnp.float32), norm_gains[0, 1])
    ffn_in = rms_scale(stream, norm_gains[0, 2]).astype(jnp.bfloat16)
    gate_proj = project_rows(ffn_in, gate_up_weight[0, 0])
    up_proj = project_rows(ffn_in, gate_up_weight[0, 1])
    active = (jax.nn.gelu(gate_proj, approximate=True) * up_proj).astype(jnp.bfloat16)
    branch = jnp.dot(active, down_weight[0], preferred_element_type=jnp.float32)
    column_count = branch.shape[1] // devices
    summed = lax.psum(branch, "tp")
    stream = stream + rms_scale(summed, norm_gains[0, 3])
    result = lax.dynamic_slice_in_dim(stream, my_index * column_count, column_count, 1)
    decode_cache = jnp.stack(written, axis=0)[None]
    return (result, decode_cache)


MESH = pl.DeviceIdType.MESH
LANES = 128
NT = (((1,), (1,)), ((), ()))
LOG_BASE = 9.210340371976184
UNROLL = True
VMEM_LIMIT = 58 * 1024 * 1024


def dot_t(left, right):
    return lax.dot_general(left, right, NT, preferred_element_type=jnp.float32)


def normed_by(vector, meansq, gain):
    return vector * lax.rsqrt(meansq + EPSILON) * (1.0 + gain)


def meansq_of(vector):
    return jnp.mean(vector * vector, axis=-1, keepdims=True)


def column_of(scalars, count):
    row = lax.broadcasted_iota(jnp.int32, (count, 1), 0)
    column = jnp.zeros((count, 1), jnp.int32)
    for i in range(count):
        column = jnp.where(row == i, scalars[i], column)
    return column.astype(jnp.float32)


def pad_rows(rows, count):
    return jnp.concatenate(
        [rows, jnp.zeros((count - rows.shape[0], rows.shape[1]), rows.dtype)], axis=0
    )


def fused_kernel(
    dims,
    len_hbm,
    table_hbm,
    hid_hbm,
    gain_hbm,
    flat_hbm,
    wq_hbm,
    wo_hbm,
    wgu_hbm,
    wd_hbm,
    out_ref,
    dec_done,
    len_ref,
    hid,
    gain,
    table,
    flat,
    wq,
    wo,
    wgu,
    wd,
    proj,
    att,
    attended,
    mix,
    branch,
    arrive,
    sums,
    squares,
    stack,
    mixed_ref,
    blend,
    page_stage,
    dec,
    load_sem,
    send_sem,
    proj_sem,
    att_sem,
    mix_sem,
    tail_sem,
):
    T, B, R, RP = dims["T"], dims["B"], dims["R"], dims["RP"]
    share, local_heads, slots = dims["share"], dims["local_heads"], dims["S"]
    per_group, groups = dims["per_group"], dims["groups"]
    planes, plane_size = dims["planes"], dims["plane_size"]
    first_owner, owner_count = dims["first_owner"], dims["owner_count"]
    width = local_heads * HEAD_DIM
    cols = wq.shape[0]
    heads_here = cols // HEAD_DIM
    q_devs = HEADS * HEAD_DIM // cols
    k_devs = KV_HEADS * HEAD_DIM // cols
    page_width = dec.shape[2]
    model = wq.shape[1]
    ff = wd.shape[0]
    chunks = model // LANES
    score_scale = (D / HEADS) ** (-0.5)
    me = lax.axis_index("tp")
    my_group = me // PREFILL_TP
    my_slot = me % PREFILL_TP
    my_plane = me // plane_size
    my_seat = me % plane_size

    def load(index, src, dst):
        return pltpu.make_async_copy(src, dst, load_sem.at[index])

    small = [
        load(0, hid_hbm, hid.at[:, pl.ds(0, model)]),
        load(1, gain_hbm, gain.at[:, pl.ds(0, model)]),
        load(2, len_hbm, len_ref),
        load(3, table_hbm, table),
    ]
    cuts = dims["cuts"]
    wq_loads = [
        load(8 + i, wq_hbm.at[:, pl.ds(lo, hi - lo)], wq.at[:, pl.ds(lo, hi - lo)])
        for i, (lo, hi) in enumerate(cuts)
    ]
    flat_load = load(4, flat_hbm, flat)
    wo_load = load(5, wo_hbm, wo)
    wgu_load = load(6, wgu_hbm, wgu)
    wd_load = load(7, wd_hbm, wd)
    for piece in small + wq_loads + [flat_load, wo_load, wgu_load, wd_load]:
        piece.start()

    barrier = pltpu.get_barrier_semaphore()

    for step in range(1, T):
        peer = lax.rem(me + step, T)
        pl.semaphore_signal(barrier, inc=1, device_id={"tp": peer}, device_id_type=MESH)

    def dec_part(ref, index):
        group, slot = index // PREFILL_TP, index % PREFILL_TP
        lane = pl.multiple_of(slot * width, width)
        return ref.at[:, pl.ds(group * per_group, per_group), :, pl.ds(lane, width)]

    def remote(src, dst, send, recv, peer):
        return pltpu.make_async_remote_copy(
            src_ref=src,
            dst_ref=dst,
            send_sem=send_sem.at[send],
            recv_sem=recv,
            device_id={"tp": peer},
            device_id_type=MESH,
        )

    def sent(send, ref):
        remote(ref, ref, send, tail_sem.at[0], me).wait_send()

    def landed(recv, ref):
        remote(ref, ref, 0, recv, me).wait_recv()

    def owners(index):
        first = index % PREFILL_TP * local_heads
        key = first // heads_here
        return (first * share // heads_here, q_devs + key, q_devs + k_devs + key)

    def proj_from(sender):
        return proj_sem.at[jnp.maximum(sender - (q_devs - 1), 0)]

    def send_proj(peer):
        remote(proj.at[me], proj.at[me], 0, proj_from(me), peer).start()

    def send_urgent():
        @pl.when(me < q_devs)
        def _():
            send_proj(me + PREFILL_TP)

        @pl.when(me >= q_devs)
        def _():
            first = (me - q_devs) % k_devs * (PREFILL_TP // k_devs)
            for g in range(groups):
                for i in range(PREFILL_TP // k_devs):
                    peer = g * PREFILL_TP + first + i
                    if g == 0:
                        send_proj(peer)
                        continue

                    @pl.when(peer != me)
                    def _():
                        send_proj(peer)

    def send_others():
        for step in range(1, T):
            peer = lax.rem(me + step, T)
            q_owner, k_owner, v_owner = owners(peer)

            @pl.when((k_owner != me) & (v_owner != me) & (me >= q_devs))
            def _():
                send_proj(peer)

    def take_proj(sender):
        @pl.when(sender != me)
        def _():
            landed(proj_from(sender), proj.at[sender])

    def push_pages(begin, end):
        for step in range(begin, min(end, T)):
            peer = lax.rem(me + step, T)
            remote(page_stage.at[peer], dec_part(dec, me), 1, tail_sem.at[3], peer).start()

    def push(send, recv, src, near_first=False):
        upper = my_plane // (planes // 2)
        for turn_of in range(planes):
            if near_first:
                plane = jnp.where(upper == 0, turn_of, planes - 1 - turn_of)
            else:
                plane = jnp.where(upper == 0, planes - 1 - turn_of, turn_of)
            for seat in range(plane_size):
                peer = plane * plane_size + lax.rem(my_seat + seat, plane_size)
                if seat:
                    remote(src, src, send, recv, peer).start()
                    continue

                @pl.when(plane != my_plane)
                def _():
                    remote(src, src, send, recv, peer).start()

    def take_plane(sems, ref, plane):
        first = plane * plane_size

        @pl.when(plane == my_plane)
        def _():
            landed(sems.at[plane], ref.at[pl.ds(first, plane_size - 1)])

        @pl.when(plane != my_plane)
        def _():
            landed(sems.at[plane], ref.at[pl.ds(first, plane_size)])

    small[2].wait()
    length = column_of(len_ref, B)
    lane = lax.broadcasted_iota(jnp.int32, (B, HEAD_DIM), 1)
    half = HEAD_DIM // 2
    exponent = (lane % half).astype(jnp.float32) * (-2.0 / HEAD_DIM)
    angles = length * jnp.exp(exponent * LOG_BASE)
    turning = jnp.broadcast_to(me < q_devs + k_devs, lane.shape)
    cosine = jnp.where(turning, jnp.cos(angles), 1.0)
    sine = jnp.where(turning, jnp.where(lane < half, -1.0, 1.0) * jnp.sin(angles), 0.0)
    small[3].wait()
    slot_page = lax.broadcasted_iota(jnp.int32, (T, slots), 1) // page_width
    spread = (slot_page == lax.broadcasted_iota(jnp.int32, (T, slots), 0)).astype(jnp.float32)
    inside = lax.broadcasted_iota(jnp.int32, (B, slots), 1) % page_width
    position = jnp.dot(
        table[...].astype(jnp.float32).astype(jnp.bfloat16),
        spread.astype(jnp.bfloat16),
        preferred_element_type=jnp.float32,
    ) * page_width + inside.astype(jnp.float32)
    request_of = lax.broadcasted_iota(jnp.int32, (B, slots), 0)

    def row_at(values, request):
        return jnp.sum(jnp.where(request_of == request, values, 0.0), axis=0, keepdims=True)

    place = [row_at(position, my_group * per_group + e) for e in range(per_group)]
    limit = [
        row_at(jnp.broadcast_to(length, (B, slots)), my_group * per_group + e)
        for e in range(per_group)
    ]
    small[0].wait()
    small[1].wait()
    stream = hid[:, :model]
    normed = normed_by(stream, meansq_of(stream), gain[0:1, :model]).astype(jnp.bfloat16)
    part = jnp.zeros((B, cols), jnp.float32)
    for (lo, hi), piece in zip(cuts, wq_loads):
        piece.wait()
        part = part + dot_t(normed[:, lo:hi], wq[:, lo:hi])
    part = part.astype(jnp.bfloat16).astype(jnp.float32)
    for head in range(heads_here):
        u = part[:, head * HEAD_DIM : (head + 1) * HEAD_DIM]
        swapped = jnp.concatenate([u[:, half:], u[:, :half]], axis=1)
        turned = u * cosine + swapped * sine
        proj[me, :, head * HEAD_DIM : (head + 1) * HEAD_DIM] = turned.astype(jnp.bfloat16)
    pl.semaphore_wait(barrier, T - 1)
    send_urgent()

    flat_load.wait()
    wanted = lax.broadcasted_iota(jnp.int32, (slots, slots), 0).astype(jnp.float32)
    for e in range(per_group):
        pick = (wanted == place[e]).astype(jnp.float32).astype(jnp.bfloat16)
        for c in range(2):
            moved = jnp.dot(pick, flat[c, e], preferred_element_type=jnp.float32)
            page_stage[:, c, e] = moved.reshape(T, page_width, width).astype(jnp.bfloat16)
    push_pages(1, dims["page_cut"])
    q_from, k_from, v_from = owners(me)
    take_proj(q_from)
    take_proj(k_from)

    rows = share * B
    row_of = lax.broadcasted_iota(jnp.int32, (rows, HEAD_DIM), 0)

    def head_of(owner, index):
        at = pl.multiple_of((index % heads_here) * HEAD_DIM, HEAD_DIM)
        return proj[owner, :, pl.ds(at, HEAD_DIM)].astype(jnp.float32)

    found = {}
    for a in range(local_heads):
        kv_head = my_slot * local_heads + a
        q = jnp.concatenate([head_of(q_from, kv_head * share + m) for m in range(share)], axis=0)
        k_new = jnp.concatenate([head_of(k_from, kv_head)] * share, axis=0)
        q16 = q.astype(jnp.bfloat16)
        own = jnp.exp(capped(jnp.sum(q * k_new, axis=-1, keepdims=True) * score_scale))
        lanes = slice(a * HEAD_DIM, (a + 1) * HEAD_DIM)
        for e in range(per_group):
            scores = dot_t(q16, flat[0, e, :, lanes]) * score_scale
            weights = jnp.where(place[e] < limit[e], jnp.exp(capped(scores)), 0.0)
            numer = jnp.dot(
                weights.astype(jnp.bfloat16),
                flat[1, e, :, lanes],
                preferred_element_type=jnp.float32,
            )
            found[a, e] = (numer, jnp.sum(weights, axis=-1, keepdims=True) + own, own)
    take_proj(v_from)
    for a in range(local_heads):
        kv_head = my_slot * local_heads + a
        v_new = jnp.concatenate([head_of(v_from, kv_head)] * share, axis=0)
        picked = [[] for m in range(share)]
        for e in range(per_group):
            request = my_group * per_group + e
            numer, denom, own = found[a, e]
            result = (numer + own.astype(jnp.bfloat16).astype(jnp.float32) * v_new) / denom
            for m in range(share):
                chosen = jnp.where(row_of == m * B + request, result, 0.0)
                picked[m].append(jnp.sum(chosen, axis=0, keepdims=True))
        for m in range(share):
            at = (a * share + m) * HEAD_DIM
            att[me, :, at : at + HEAD_DIM] = jnp.concatenate(picked[m], axis=0).astype(jnp.bfloat16)
    push(2, att_sem.at[my_plane], att.at[me])
    send_others()

    first_lane = pl.multiple_of(me * R // LANES * LANES, LANES)
    window = RP + LANES
    turn = window - lax.rem(me * R, LANES)
    own_hid = pltpu.roll(hid[:, pl.ds(first_lane, window)], turn, 1)[:, :RP]
    own_gain = pltpu.roll(gain[:, pl.ds(first_lane, window)], turn, 1)[:, :RP]
    wo_load.wait()
    q_width = att.shape[2]
    halves = T // PREFILL_TP
    slots_half = PREFILL_TP // halves
    half_width = slots_half * q_width
    for p in range(planes):
        take_plane(att_sem, att, jnp.int32(p))
    pieces = [
        jnp.concatenate(
            [att[g * PREFILL_TP + s].astype(jnp.float32) for g in range(groups)], axis=0
        )
        for s in range(PREFILL_TP)
    ]
    probe = pad_rows(jnp.concatenate(pieces, axis=1).astype(jnp.bfloat16), SUBLANES)
    pair = R // 2
    pair_lane = pair // LANES * LANES
    cut = probe.shape[1] // 2
    sides = [
        dot_t(
            jnp.concatenate([probe[:, k : k + cut], wo[pair:, k : k + cut]], axis=0),
            jnp.concatenate([wo[:pair, k : k + cut], probe[:, k : k + cut]], axis=0),
        )
        for k in (0, cut)
    ]
    flatwise = jnp.concatenate([side[:B, :pair] for side in sides], axis=0)
    flatwise = flatwise[:B] + flatwise[B:]
    upward = [
        jnp.concatenate(
            [
                side[SUBLANES:, pair_lane:],
                jnp.zeros((pair, LANES - (SUBLANES + pair - pair_lane)), jnp.float32),
            ],
            axis=1,
        ).T[pair - pair_lane : pair - pair_lane + B]
        for side in sides
    ]
    mixed = jnp.concatenate([flatwise, upward[0] + upward[1]], axis=1)
    mixed = mixed.astype(jnp.bfloat16).astype(jnp.float32)
    mixed = jnp.concatenate([mixed, jnp.zeros((B, RP - R), jnp.float32)], axis=1)
    shift = dims["seat_shift"]
    mix[me] = pltpu.roll(mixed, my_seat * shift, 1).astype(jnp.bfloat16)
    push(3, mix_sem.at[my_plane], mix.at[me], True)
    blend[:B, :] = hid[:, :model] * (1.0 + gain[2:3, :model])
    wgu_load.wait()
    side = ff // 2
    tile = dims["ff_tile"]
    at_lane = tile // LANES * LANES
    blocks = [(s, c) for s in range(side // tile) for c in range(2)]
    half_cols = model // halves
    half_seats = T // halves
    front, upright = {}, {}
    for turn_of in range(halves):
        which = (my_plane // (planes // halves) + turn_of) % halves
        for p in range(planes // halves):
            plane = which * (planes // halves) + p
            if turn_of:
                landed(mix_sem.at[plane], mix.at[pl.ds(plane * plane_size, plane_size)])
            else:
                take_plane(mix_sem, mix, plane)
        if turn_of == 0:
            push_pages(dims["page_cut"], T)
        tiles = [None] * (half_cols // LANES)
        for s in range(half_seats):
            block = mix[which * half_seats + s].astype(jnp.float32)
            for i in range(RP // LANES):
                at = s * R // LANES + i
                piece = block[:, i * LANES : (i + 1) * LANES]
                if at < len(tiles):
                    tiles[at] = piece if tiles[at] is None else tiles[at] + piece
        got = jnp.concatenate(tiles, axis=1)
        span_at = pl.ds(pl.multiple_of(which * half_cols, LANES), half_cols)
        mixed_ref[:, span_at] = got
        blend[B:, span_at] = got * ((1.0 + gain[1:2, span_at]) * (1.0 + gain[2:3, span_at]))
        exact = blend[:, span_at]
        high = exact.astype(jnp.bfloat16).astype(jnp.float32)
        probe = jnp.concatenate([high, exact - high], axis=0).astype(jnp.bfloat16)
        if turn_of == halves - 1:
            mixed_all = mixed_ref[...]
            mixed_ms = meansq_of(mixed_all)
            stream = hid[:, :model] + normed_by(mixed_all, mixed_ms, gain[1:2, :model])
            outer = lax.rsqrt(meansq_of(stream) + EPSILON)
            inner = lax.rsqrt(mixed_ms + EPSILON)
            mine = own_hid + normed_by(mixed, mixed_ms, own_gain[1:2, :])
        for s, c in blocks:
            at = s * tile
            pushed = jnp.concatenate([wgu[c, at : at + tile, span_at], probe], axis=0)
            passed = jnp.concatenate(
                [probe, wgu[c, side + at : side + at + tile, span_at]], axis=0
            )
            both = dot_t(passed, pushed)
            part = both[: 2 * B, :tile] + both[2 * B : 4 * B, :tile]
            front[s, c] = part if turn_of == 0 else front[s, c] + part
            rest = both[4 * B :, at_lane:]
            wide = rest.shape[1]
            if turn_of < halves - 1:
                stack[s, c, :, :wide] = rest
            else:
                rest = jnp.concatenate(
                    [rest + stack[s, c, :, :wide], jnp.zeros((tile, LANES - wide), jnp.float32)],
                    axis=1,
                )
                turned = rest.T
                first = tile - at_lane
                upright[s, c] = turned[first : first + 2 * B] + turned[first + 2 * B : first + 4 * B]

    def settle(parts):
        return outer * (parts[:B] + inner * parts[B:])

    steps = range(side // tile)
    active = []
    for table_of in (front, upright):
        for s in steps:
            gate, up = settle(table_of[s, 0]), settle(table_of[s, 1])
            active.append(jax.nn.gelu(gate, approximate=True) * up)
    active = jnp.concatenate(active, axis=1).astype(jnp.bfloat16)
    wd_load.wait()
    owned = model // owner_count
    span = arrive.shape[2]
    is_owner = (me >= first_owner) & (me < first_owner + owner_count)
    side_owners = owner_count // halves
    for turn_of in range(halves):
        which = (halves - 1 - my_plane // (planes // halves) + turn_of) % halves
        half_at = pl.multiple_of(which * half_cols, LANES)
        wide = -(-half_cols // (4 * LANES)) * 4 * LANES
        done_cols = wide if turn_of == 0 else model - wide
        done_at = pl.multiple_of(which * (model - done_cols), LANES)
        part = jnp.dot(active, wd[:, pl.ds(done_at, done_cols)], preferred_element_type=jnp.float32)
        branch[:, pl.ds(done_at, done_cols)] = part.astype(jnp.bfloat16)
        for i in range(side_owners):
            peer = first_owner + which * side_owners + i

            @pl.when(me != peer)
            def _():
                begin = pl.multiple_of(half_at + i * owned // LANES * LANES, LANES)
                remote(branch.at[:, pl.ds(begin, span)], arrive.at[me], 4, tail_sem.at[0], peer).start()

    @pl.when(is_owner)
    def _():
        o = me - first_owner
        odd = o % 2
        base = pl.multiple_of(o * owned // LANES * LANES, LANES)
        total = branch[:, pl.ds(base, span)].astype(jnp.float32)
        landed(tail_sem.at[0], arrive.at[pl.ds(0, T - 1)])
        for s in range(T):
            piece = arrive[s].astype(jnp.float32)
            total = total + jnp.where(me == s, 0.0, piece)
        offset = odd * (LANES // 2)
        lane_of = lax.broadcasted_iota(jnp.int32, (B, span), 1)
        inside = (lane_of >= offset) & (lane_of < offset + owned)
        kept = jnp.where(inside, total, 0.0)
        ready = []
        for i in range(2):
            begin = i * R // LANES * LANES
            left = RP - (i * R - begin) - offset
            ready.append(pltpu.roll(kept[:, begin : begin + RP], lax.rem(left, RP), 1))
            sums[i] = ready[i]
        for i in range(2):
            peer = o * 2 + i

            @pl.when(peer != me)
            def _():
                remote(sums.at[i], sums.at[2], 5, tail_sem.at[1], peer).start()

            @pl.when(peer == me)
            def _():
                sums[2] = ready[i]

        each = jnp.sum(kept * kept, axis=-1, keepdims=True)
        spot = lax.broadcasted_iota(jnp.int32, (B, LANES), 1) == lax.broadcasted_iota(
            jnp.int32, (B, LANES), 0
        )
        squares[o] = jnp.sum(jnp.where(spot, each, 0.0), axis=0, keepdims=True)
        push(6, tail_sem.at[2], squares.at[o])

    dec_part(dec, me)[...] = page_stage[me]
    landed(tail_sem.at[3], page_stage.at[pl.ds(0, T - 1)])
    for owner in range(q_devs, q_devs + 2 * k_devs):
        @pl.when((owner != k_from) & (owner != v_from))
        def _():
            take_proj(jnp.int32(owner))

    token = lax.broadcasted_iota(jnp.int32, (page_width, cols), 0) + me * page_width
    for c in range(2):
        for i in range(k_devs):
            fresh = proj[q_devs + c * k_devs + i].astype(jnp.float32)
            for r in range(B):
                old = dec[c, r, :, i * cols : (i + 1) * cols].astype(jnp.float32)
                row = jnp.broadcast_to(fresh[r : r + 1, :], old.shape)
                new = jnp.where(token == len_ref[r], row, old)
                dec_done[c, r, :, i * cols : (i + 1) * cols] = new.astype(jnp.bfloat16)

    for send, ref in ((2, att), (3, mix)):
        sent(send, ref.at[pl.ds(0, T - 1)])
    sent(1, page_stage.at[pl.ds(0, T - 1)])

    @pl.when(me < q_devs)
    def _():
        sent(0, proj.at[0])

    @pl.when(me >= q_devs)
    def _():
        sent(0, proj.at[pl.ds(0, T - 1)])

    @pl.when(is_owner)
    def _():
        sent(4, arrive.at[pl.ds(0, owner_count - 1)])
        landed(tail_sem.at[2], squares.at[pl.ds(0, owner_count - 1)])

    @pl.when(jnp.logical_not(is_owner))
    def _():
        sent(4, arrive.at[pl.ds(0, owner_count)])
        landed(tail_sem.at[2], squares.at[pl.ds(0, owner_count)])

    @pl.when(first_owner + me // 2 != me)
    def _():
        landed(tail_sem.at[1], sums.at[2])

    sumsq = squares[0]
    for s in range(1, owner_count):
        sumsq = sumsq + squares[s]
    spot = lax.broadcasted_iota(jnp.int32, (B, LANES), 1) == lax.broadcasted_iota(
        jnp.int32, (B, LANES), 0
    )
    branch_ms = jnp.sum(
        jnp.where(spot, jnp.broadcast_to(sumsq, (B, LANES)), 0.0), axis=-1, keepdims=True
    ) * (1.0 / model)
    result = mine + normed_by(sums[2], branch_ms, own_gain[3:4, :])
    out_ref[...] = result[:, :R]

    @pl.when(is_owner)
    def _():
        o = me - first_owner
        sent(6, arrive_like(squares, T - 1, owner_count))

        @pl.when(o * 2 == me)
        def _():
            sent(5, sums.at[0])

        @pl.when(o * 2 + 1 == me)
        def _():
            sent(5, sums.at[0])

        @pl.when((o * 2 != me) & (o * 2 + 1 != me))
        def _():
            sent(5, sums.at[pl.ds(0, 2)])


def arrive_like(squares, count, limit):
    return squares.at[pl.ds(0, count)]


def finish_kernel(out_ref, dec_ref, out_hbm, dec_hbm, sem):
    first = pltpu.make_async_copy(dec_ref, dec_hbm, sem.at[0])
    second = pltpu.make_async_copy(out_ref, out_hbm, sem.at[1])
    first.start()
    second.start()
    first.wait()
    second.wait()


def fits_kernel(shapes, devices):
    batch_rows, model = shapes["hidden"]
    cols, rows, ff = shapes["qkv"], shapes["out"], shapes["ff"]
    groups = devices // PREFILL_TP
    weight_bytes = 2 * (cols * model + rows * HEADS * HEAD_DIM + 3 * ff * model)
    return (
        devices == 2 * PREFILL_TP
        and cols == HEADS // PREFILL_TP * HEAD_DIM
        and (KV_HEADS * HEAD_DIM) % cols == 0
        and (HEADS * HEAD_DIM) % cols == 0
        and batch_rows % groups == 0
        and model % (LANES * 2) == 0
        and ff % (6 * SUBLANES) == 0
        and rows * devices == model
        and rows * 4 % LANES == 0
        and rows % (2 * SUBLANES) == 0
        and weight_bytes < VMEM_LIMIT * 3 // 4
        and batch_rows == 4
    )


SUBLANES = 16


def fused_device(
    hidden_in,
    prefill_cache,
    lengths,
    page_table,
    qkv_weight,
    out_weight,
    gate_up_weight,
    down_weight,
    norm_gains,
):
    T = lax.axis_size("tp")
    B, model = hidden_in.shape
    groups = T // PREFILL_TP
    per_group = B // groups
    local_heads = KV_HEADS // PREFILL_TP
    share = HEADS // KV_HEADS
    pages, page_width, width = prefill_cache.shape[4:]
    S = pages * page_width
    cols = qkv_weight.shape[1]
    R = out_weight.shape[1]
    RP = -(-R // LANES) * LANES
    ff = down_weight.shape[1]
    k_cols = KV_HEADS * HEAD_DIM
    planes = 4
    plane_size = T // planes
    owner_count = T // 2
    depth = model // 256
    marks = list(range(0, depth, 2)) + [depth]
    dims = dict(
        T=T, B=B, R=R, RP=RP, S=S, share=share, local_heads=local_heads,
        per_group=per_group, groups=groups, planes=planes, plane_size=plane_size,
        first_owner=plane_size, owner_count=owner_count, seat_shift=R % LANES,
        cuts=[(lo * 256, hi * 256) for lo, hi in zip(marks, marks[1:])],
        ff_tile=ff // 6, page_cut=T // 2,
    )
    q_width = local_heads * share * HEAD_DIM
    span = -(-(model // owner_count) // LANES) * LANES
    bf16, f32 = jnp.bfloat16, jnp.float32
    vmem = pl.BlockSpec(memory_space=pltpu.VMEM)
    anyw = pl.BlockSpec(memory_space=pl.ANY)
    out, dec = pl.pallas_call(
        functools.partial(fused_kernel, dims),
        out_shape=(
            pltpu.VMEM((B, R), f32),
            pltpu.VMEM((2, B, page_width, k_cols), bf16),
        ),
        in_specs=[anyw] * 9,
        out_specs=(vmem, vmem),
        scratch_shapes=[
            pltpu.SMEM((B,), jnp.int32),
            pltpu.VMEM((B, model + RP), f32),
            pltpu.VMEM((norm_gains.shape[1], model + RP), f32),
            pltpu.VMEM((B, T), jnp.int32),
            pltpu.VMEM((2, per_group, S, width), bf16),
            pltpu.VMEM((cols, model), bf16),
            pltpu.VMEM((R, HEADS * HEAD_DIM), bf16),
            pltpu.VMEM((2, ff, model), bf16),
            pltpu.VMEM((ff, model), bf16),
            pltpu.VMEM((T, B, cols), bf16),
            pltpu.VMEM((T, per_group, q_width), bf16),
            pltpu.VMEM((B, HEADS * HEAD_DIM), bf16),
            pltpu.VMEM((T, B, RP), bf16),
            pltpu.VMEM((B, model), bf16),
            pltpu.VMEM((T, B, span), bf16),
            pltpu.VMEM((3, B, RP), f32),
            pltpu.VMEM((T, 1, LANES), f32),
            pltpu.VMEM((3, 2, ff // 6, LANES), f32),
            pltpu.VMEM((B, model), f32),
            pltpu.VMEM((2 * B, model), f32),
            pltpu.VMEM((T, 2, per_group, page_width, width), bf16),
            pltpu.VMEM((2, B, page_width, k_cols), bf16),
            pltpu.SemaphoreType.DMA((8 + len(dims["cuts"]),)),
            pltpu.SemaphoreType.DMA((7,)),
            pltpu.SemaphoreType.DMA((9,)),
            pltpu.SemaphoreType.DMA((4,)),
            pltpu.SemaphoreType.DMA((4,)),
            pltpu.SemaphoreType.DMA((4,)),
        ],
        compiler_params=pltpu.CompilerParams(
            collective_id=0, has_side_effects=True, vmem_limit_bytes=VMEM_LIMIT
        ),
    )(
        lengths,
        page_table,
        hidden_in,
        norm_gains[0],
        prefill_cache.reshape(2, per_group, S, width),
        qkv_weight[0],
        out_weight[0],
        gate_up_weight[0],
        down_weight[0],
    )
    out, dec = pl.pallas_call(
        finish_kernel,
        out_shape=(
            jax.ShapeDtypeStruct((B, R), f32),
            jax.ShapeDtypeStruct((2, B, page_width, k_cols), bf16),
        ),
        in_specs=[vmem, vmem],
        out_specs=(anyw, anyw),
        scratch_shapes=[pltpu.SemaphoreType.DMA((2,))],
    )(
        pltpu.with_memory_space_constraint(out, pltpu.VMEM),
        pltpu.with_memory_space_constraint(dec, pltpu.VMEM),
    )
    return out, dec.reshape(1, 1, 2, B, page_width, k_cols)


def step(*args):
    shapes = {
        "hidden": args[0].shape,
        "qkv": args[4].shape[1],
        "out": args[5].shape[1],
        "ff": args[7].shape[1],
    }
    chosen = fused_device if fits_kernel(shapes, lax.axis_size("tp")) else on_device
    return chosen(*args)


def solution(mesh):
    placed = (
        P("grp", None),
        P("tp", None, None, "grp", None, None, None),
        P("grp"),
        P("grp", None),
        P(None, "tp", None),
        P(None, "tp", None),
        P(None, None, "tp", None),
        P(None, "tp", None),
        P(),
    )
    return jax.shard_map(
        step,
        mesh=mesh,
        in_specs=placed,
        out_specs=(P("grp", "tp"), P("tp", None, None, "grp", None, None)),
        check_vma=False,
    )
```

```python
import functools

import jax
import jax.numpy as jnp
from jax import lax
from jax.experimental import pallas as pl
from jax.experimental.pallas import tpu as pltpu
from jax.sharding import PartitionSpec as P

D = 4608
HEADS = 32
KV_HEADS = 16
HEAD_DIM = 128
PREFILL_TP = 8


EPSILON = 1e-06
SOFTCAP = 50.0


def rms_scale(vector, gain_row):
    meansq = jnp.mean(vector * vector, axis=-1, keepdims=True)
    return vector * lax.rsqrt(meansq + EPSILON) * (1.0 + gain_row)


def rotate(vector, positions):
    half_dim = vector.shape[-1] // 2
    exponent = jnp.arange(half_dim, dtype=jnp.float32) * (-2.0 / vector.shape[-1])
    frequency = jnp.power(jnp.float32(10000.0), exponent)
    angles = positions.astype(jnp.float32)[:, None, None] * frequency
    cosine = jnp.cos(angles)
    sine_term = jnp.sin(angles)
    front_half = vector[..., :half_dim]
    back_half = vector[..., half_dim:]
    return jnp.concatenate(
        [front_half * cosine - back_half * sine_term, back_half * cosine + front_half * sine_term],
        axis=-1,
    )


def capped(raw_scores):
    return SOFTCAP * jnp.tanh(raw_scores / SOFTCAP)


def round_back(vector):
    return lax.optimization_barrier(vector.astype(jnp.bfloat16)).astype(jnp.float32)


def pick_slot(vector, my_group, my_slot):
    inner = lax.dynamic_index_in_dim(vector, my_group, 0, False)
    return lax.dynamic_index_in_dim(inner, my_slot, 1, False)


def take_pages(page_block, page_order):
    return jnp.take(page_block, page_order, axis=2)


def project_rows(left, weight_rows):
    return jnp.einsum("bd,cd->bc", left, weight_rows, preferred_element_type=jnp.float32)


def on_device(
    hidden_in,
    prefill_cache,
    lengths,
    page_table,
    qkv_weight,
    out_weight,
    gate_up_weight,
    down_weight,
    norm_gains,
):
    devices = lax.axis_size("tp")
    my_index = lax.axis_index("tp")
    batch_rows = hidden_in.shape[0]
    groups = devices // PREFILL_TP
    per_group = batch_rows // groups
    local_heads = KV_HEADS // PREFILL_TP
    head_share = HEADS // KV_HEADS
    layer_count = prefill_cache.shape[1]
    page_width = prefill_cache.shape[5]
    score_scale = (D / HEADS) ** (-0.5)
    q_cols = HEADS * HEAD_DIM
    k_cols = KV_HEADS * HEAD_DIM
    my_group = my_index // PREFILL_TP
    my_slot = my_index % PREFILL_TP
    group_rows = lax.dynamic_slice_in_dim(page_table, my_group * per_group, per_group, 0)
    group_lengths = lax.dynamic_slice_in_dim(lengths, my_group * per_group, per_group, 0)
    local_cache = prefill_cache[0]
    page_ids = jnp.arange(devices, dtype=jnp.int32)
    onehot = (group_rows[:, :, None] == page_ids[None, None, :]).astype(jnp.int32)
    inverse = jnp.sum(onehot * page_ids[None, :, None], axis=1)
    arranged = jax.vmap(take_pages, in_axes=(2, 0), out_axes=2)(local_cache, inverse)
    relaid = lax.all_to_all(arranged, "tp", split_axis=3, concat_axis=3, tiled=True)
    relaid = relaid.reshape(
        layer_count, 2, per_group, groups, PREFILL_TP, page_width, local_heads, HEAD_DIM
    )
    decode_local = relaid.transpose(0, 1, 3, 2, 5, 4, 6, 7).reshape(
        layer_count, 2, batch_rows, page_width, k_cols
    )
    my_pos = my_index * page_width + jnp.arange(page_width, dtype=jnp.int32)
    fresh_slot = my_pos[None, :] == lengths[:, None]
    kept_cache = local_cache.reshape(
        layer_count, 2, per_group, devices, page_width, local_heads, HEAD_DIM
    )
    cache_pos = (
        group_rows[:, :, None] * page_width + jnp.arange(page_width, dtype=jnp.int32)[None, None, :]
    )
    kept_visible = cache_pos < group_lengths[:, None, None]
    stream = hidden_in
    normed = rms_scale(stream, norm_gains[0, 0]).astype(jnp.bfloat16)
    column_part = project_rows(normed, qkv_weight[0]).astype(jnp.bfloat16)
    projected = lax.all_gather(column_part, "tp", axis=1, tiled=True)
    queries = rotate(
        projected[:, :q_cols].astype(jnp.float32).reshape(batch_rows, HEADS, HEAD_DIM), lengths
    ).astype(jnp.bfloat16)
    new_key = rotate(
        projected[:, q_cols : q_cols + k_cols]
        .astype(jnp.float32)
        .reshape(batch_rows, KV_HEADS, HEAD_DIM),
        lengths,
    ).astype(jnp.bfloat16)
    new_value = projected[:, q_cols + k_cols :]
    key_layer = jnp.where(
        fresh_slot[:, :, None], new_key.reshape(batch_rows, 1, k_cols), decode_local[0, 0]
    )
    value_layer = jnp.where(
        fresh_slot[:, :, None], new_value.reshape(batch_rows, 1, k_cols), decode_local[0, 1]
    )
    written = [jnp.stack([key_layer, value_layer], axis=0)]
    flat_q = queries.reshape(batch_rows, KV_HEADS, head_share, HEAD_DIM)
    flat_k = new_key.reshape(batch_rows, KV_HEADS, 1, HEAD_DIM)
    flat_v = new_value.reshape(batch_rows, KV_HEADS, 1, HEAD_DIM)
    own_weight = jnp.exp(
        capped(
            jnp.sum(flat_q.astype(jnp.float32) * flat_k.astype(jnp.float32), axis=-1) * score_scale
        )
    )
    own_term = round_back(own_weight)[..., None] * flat_v.astype(jnp.float32)
    shaped_q = flat_q.reshape(groups, per_group, PREFILL_TP, local_heads, head_share, HEAD_DIM)
    shaped_own = own_weight.reshape(groups, per_group, PREFILL_TP, local_heads, head_share)
    shaped_term = own_term.reshape(groups, per_group, PREFILL_TP, local_heads, head_share, HEAD_DIM)
    my_queries = pick_slot(shaped_q, my_group, my_slot)
    cached_keys = kept_cache[0, 0]
    cached_values = kept_cache[0, 1]
    raw_scores = (
        jnp.einsum("ramd,rjcad->ramjc", my_queries, cached_keys, preferred_element_type=jnp.float32)
        * score_scale
    )
    weights = jnp.where(kept_visible[:, None, None, :, :], jnp.exp(capped(raw_scores)), 0.0)
    numerator = jnp.einsum(
        "ramjc,rjcad->ramd",
        weights.astype(jnp.bfloat16),
        cached_values,
        preferred_element_type=jnp.float32,
    )
    numerator = numerator + pick_slot(shaped_term, my_group, my_slot)
    denominator = jnp.sum(weights, axis=(-2, -1)) + pick_slot(shaped_own, my_group, my_slot)
    mine = (
        (numerator / denominator[..., None])
        .astype(jnp.bfloat16)
        .reshape(1, per_group, local_heads * head_share * HEAD_DIM)
    )
    gathered = lax.all_gather(mine, "tp", axis=0, tiled=True)
    attended = (
        gathered.reshape(groups, PREFILL_TP, per_group, local_heads * head_share * HEAD_DIM)
        .transpose(0, 2, 1, 3)
        .reshape(batch_rows, q_cols)
    )
    mixed_part = project_rows(attended, out_weight[0]).astype(jnp.bfloat16)
    mixed_out = lax.all_gather(mixed_part, "tp", axis=1, tiled=True)
    stream = stream + rms_scale(mixed_out.astype(jnp.float32), norm_gains[0, 1])
    ffn_in = rms_scale(stream, norm_gains[0, 2]).astype(jnp.bfloat16)
    gate_proj = project_rows(ffn_in, gate_up_weight[0, 0])
    up_proj = project_rows(ffn_in, gate_up_weight[0, 1])
    active = (jax.nn.gelu(gate_proj, approximate=True) * up_proj).astype(jnp.bfloat16)
    branch = jnp.dot(active, down_weight[0], preferred_element_type=jnp.float32)
    column_count = branch.shape[1] // devices
    summed = lax.psum(branch, "tp")
    stream = stream + rms_scale(summed, norm_gains[0, 3])
    result = lax.dynamic_slice_in_dim(stream, my_index * column_count, column_count, 1)
    decode_cache = jnp.stack(written, axis=0)[None]
    return (result, decode_cache)


MESH = pl.DeviceIdType.MESH
LANES = 128
NT = (((1,), (1,)), ((), ()))
LOG_BASE = 9.210340371976184
UNROLL = True
VMEM_LIMIT = 58 * 1024 * 1024


def dot_t(left, right):
    return lax.dot_general(left, right, NT, preferred_element_type=jnp.float32)


def normed_by(vector, meansq, gain):
    return vector * lax.rsqrt(meansq + EPSILON) * (1.0 + gain)


def meansq_of(vector):
    return jnp.mean(vector * vector, axis=-1, keepdims=True)


def column_of(scalars, count):
    row = lax.broadcasted_iota(jnp.int32, (count, 1), 0)
    column = jnp.zeros((count, 1), jnp.int32)
    for i in range(count):
        column = jnp.where(row == i, scalars[i], column)
    return column.astype(jnp.float32)


def pad_rows(rows, count):
    return jnp.concatenate(
        [rows, jnp.zeros((count - rows.shape[0], rows.shape[1]), rows.dtype)], axis=0
    )


def fused_kernel(
    dims,
    len_hbm,
    table_hbm,
    hid_hbm,
    gain_hbm,
    flat_hbm,
    wq_hbm,
    wo_hbm,
    wgu_hbm,
    wd_hbm,
    out_ref,
    dec_done,
    len_ref,
    hid,
    gain,
    table,
    flat,
    wq,
    wo,
    wgu,
    wd,
    proj,
    att,
    attended,
    mix,
    branch,
    arrive,
    sums,
    squares,
    stack,
    mixed_ref,
    blend,
    page_stage,
    dec,
    load_sem,
    send_sem,
    proj_sem,
    att_sem,
    mix_sem,
    tail_sem,
):
    T, B, R, RP = dims["T"], dims["B"], dims["R"], dims["RP"]
    share, local_heads, slots = dims["share"], dims["local_heads"], dims["S"]
    per_group, groups = dims["per_group"], dims["groups"]
    planes, plane_size = dims["planes"], dims["plane_size"]
    first_owner, owner_count = dims["first_owner"], dims["owner_count"]
    width = local_heads * HEAD_DIM
    cols = wq.shape[0]
    heads_here = cols // HEAD_DIM
    q_devs = HEADS * HEAD_DIM // cols
    k_devs = KV_HEADS * HEAD_DIM // cols
    page_width = dec.shape[2]
    model = wq.shape[1]
    ff = wd.shape[0]
    chunks = model // LANES
    score_scale = (D / HEADS) ** (-0.5)
    me = lax.axis_index("tp")
    my_group = me // PREFILL_TP
    my_slot = me % PREFILL_TP
    my_plane = me // plane_size
    my_seat = me % plane_size

    def load(index, src, dst):
        return pltpu.make_async_copy(src, dst, load_sem.at[index])

    small = [
        load(0, hid_hbm, hid.at[:, pl.ds(0, model)]),
        load(1, gain_hbm, gain.at[:, pl.ds(0, model)]),
        load(2, len_hbm, len_ref),
        load(3, table_hbm, table),
    ]
    cuts = dims["cuts"]
    wq_loads = [
        load(8 + i, wq_hbm.at[:, pl.ds(lo, hi - lo)], wq.at[:, pl.ds(lo, hi - lo)])
        for i, (lo, hi) in enumerate(cuts)
    ]
    flat_load = load(4, flat_hbm, flat)
    wo_load = load(5, wo_hbm, wo)
    wgu_load = load(6, wgu_hbm, wgu)
    wd_load = load(7, wd_hbm, wd)
    for piece in small + wq_loads + [flat_load, wo_load, wgu_load, wd_load]:
        piece.start()

    barrier = pltpu.get_barrier_semaphore()

    for step in range(1, T):
        peer = lax.rem(me + step, T)
        pl.semaphore_signal(barrier, inc=1, device_id={"tp": peer}, device_id_type=MESH)

    def dec_part(ref, index):
        group, slot = index // PREFILL_TP, index % PREFILL_TP
        lane = pl.multiple_of(slot * width, width)
        return ref.at[:, pl.ds(group * per_group, per_group), :, pl.ds(lane, width)]

    def remote(src, dst, send, recv, peer):
        return pltpu.make_async_remote_copy(
            src_ref=src,
            dst_ref=dst,
            send_sem=send_sem.at[send],
            recv_sem=recv,
            device_id={"tp": peer},
            device_id_type=MESH,
        )

    def sent(send, ref):
        remote(ref, ref, send, tail_sem.at[0], me).wait_send()

    def landed(recv, ref):
        remote(ref, ref, 0, recv, me).wait_recv()

    def owners(index):
        first = index % PREFILL_TP * local_heads
        key = first // heads_here
        return (first * share // heads_here, q_devs + key, q_devs + k_devs + key)

    def proj_from(sender):
        return proj_sem.at[jnp.maximum(sender - (q_devs - 1), 0)]

    def send_proj(peer):
        remote(proj.at[me], proj.at[me], 0, proj_from(me), peer).start()

    def send_urgent():
        @pl.when(me < q_devs)
        def _():
            send_proj(me + PREFILL_TP)

        @pl.when(me >= q_devs)
        def _():
            first = (me - q_devs) % k_devs * (PREFILL_TP // k_devs)
            for g in range(groups):
                for i in range(PREFILL_TP // k_devs):
                    peer = g * PREFILL_TP + first + i
                    if g == 0:
                        send_proj(peer)
                        continue

                    @pl.when(peer != me)
                    def _():
                        send_proj(peer)

    def send_others():
        for step in range(1, T):
            peer = lax.rem(me + step, T)
            q_owner, k_owner, v_owner = owners(peer)

            @pl.when((k_owner != me) & (v_owner != me) & (me >= q_devs))
            def _():
                send_proj(peer)

    def take_proj(sender):
        @pl.when(sender != me)
        def _():
            landed(proj_from(sender), proj.at[sender])

    def push_pages(begin, end):
        for step in range(begin, min(end, T)):
            peer = lax.rem(me + step, T)
            remote(page_stage.at[peer], dec_part(dec, me), 1, tail_sem.at[3], peer).start()

    def push(send, recv, src, near_first=False):
        upper = my_plane // (planes // 2)
        for turn_of in range(planes):
            if near_first:
                plane = jnp.where(upper == 0, turn_of, planes - 1 - turn_of)
            else:
                plane = jnp.where(upper == 0, planes - 1 - turn_of, turn_of)
            for seat in range(plane_size):
                peer = plane * plane_size + lax.rem(my_seat + seat, plane_size)
                if seat:
                    remote(src, src, send, recv, peer).start()
                    continue

                @pl.when(plane != my_plane)
                def _():
                    remote(src, src, send, recv, peer).start()

    small[2].wait()
    length = column_of(len_ref, B)
    lane = lax.broadcasted_iota(jnp.int32, (B, HEAD_DIM), 1)
    half = HEAD_DIM // 2
    exponent = (lane % half).astype(jnp.float32) * (-2.0 / HEAD_DIM)
    angles = length * jnp.exp(exponent * LOG_BASE)
    turning = jnp.broadcast_to(me < q_devs + k_devs, lane.shape)
    cosine = jnp.where(turning, jnp.cos(angles), 1.0)
    sine = jnp.where(turning, jnp.where(lane < half, -1.0, 1.0) * jnp.sin(angles), 0.0)
    small[3].wait()
    slot_page = lax.broadcasted_iota(jnp.int32, (T, slots), 1) // page_width
    spread = (slot_page == lax.broadcasted_iota(jnp.int32, (T, slots), 0)).astype(jnp.float32)
    inside = lax.broadcasted_iota(jnp.int32, (B, slots), 1) % page_width
    position = jnp.dot(
        table[...].astype(jnp.float32).astype(jnp.bfloat16),
        spread.astype(jnp.bfloat16),
        preferred_element_type=jnp.float32,
    ) * page_width + inside.astype(jnp.float32)
    request_of = lax.broadcasted_iota(jnp.int32, (B, slots), 0)

    def row_at(values, request):
        return jnp.sum(jnp.where(request_of == request, values, 0.0), axis=0, keepdims=True)

    place = [row_at(position, my_group * per_group + e) for e in range(per_group)]
    limit = [
        row_at(jnp.broadcast_to(length, (B, slots)), my_group * per_group + e)
        for e in range(per_group)
    ]
    small[0].wait()
    small[1].wait()
    stream = hid[:, :model]
    normed = normed_by(stream, meansq_of(stream), gain[0:1, :model]).astype(jnp.bfloat16)
    part = jnp.zeros((B, cols), jnp.float32)
    for (lo, hi), piece in zip(cuts, wq_loads):
        piece.wait()
        part = part + dot_t(normed[:, lo:hi], wq[:, lo:hi])
    part = part.astype(jnp.bfloat16).astype(jnp.float32)
    for head in range(heads_here):
        u = part[:, head * HEAD_DIM : (head + 1) * HEAD_DIM]
        swapped = jnp.concatenate([u[:, half:], u[:, :half]], axis=1)
        turned = u * cosine + swapped * sine
        proj[me, :, head * HEAD_DIM : (head + 1) * HEAD_DIM] = turned.astype(jnp.bfloat16)
    pl.semaphore_wait(barrier, T - 1)
    send_urgent()

    flat_load.wait()
    wanted = lax.broadcasted_iota(jnp.int32, (slots, slots), 0).astype(jnp.float32)
    for e in range(per_group):
        pick = (wanted == place[e]).astype(jnp.float32).astype(jnp.bfloat16)
        for c in range(2):
            moved = jnp.dot(pick, flat[c, e], preferred_element_type=jnp.float32)
            page_stage[:, c, e] = moved.reshape(T, page_width, width).astype(jnp.bfloat16)
    push_pages(1, dims["page_cut"])
    q_from, k_from, v_from = owners(me)
    take_proj(q_from)
    take_proj(k_from)

    rows = share * B
    row_of = lax.broadcasted_iota(jnp.int32, (rows, HEAD_DIM), 0)

    def head_of(owner, index):
        at = pl.multiple_of((index % heads_here) * HEAD_DIM, HEAD_DIM)
        return proj[owner, :, pl.ds(at, HEAD_DIM)].astype(jnp.float32)

    found = {}
    for a in range(local_heads):
        kv_head = my_slot * local_heads + a
        q = jnp.concatenate([head_of(q_from, kv_head * share + m) for m in range(share)], axis=0)
        k_new = jnp.concatenate([head_of(k_from, kv_head)] * share, axis=0)
        q16 = q.astype(jnp.bfloat16)
        own = jnp.exp(capped(jnp.sum(q * k_new, axis=-1, keepdims=True) * score_scale))
        lanes = slice(a * HEAD_DIM, (a + 1) * HEAD_DIM)
        for e in range(per_group):
            scores = dot_t(q16, flat[0, e, :, lanes]) * score_scale
            weights = jnp.where(place[e] < limit[e], jnp.exp(capped(scores)), 0.0)
            numer = jnp.dot(
                weights.astype(jnp.bfloat16),
                flat[1, e, :, lanes],
                preferred_element_type=jnp.float32,
            )
            found[a, e] = (numer, jnp.sum(weights, axis=-1, keepdims=True) + own, own)
    take_proj(v_from)
    for a in range(local_heads):
        kv_head = my_slot * local_heads + a
        v_new = jnp.concatenate([head_of(v_from, kv_head)] * share, axis=0)
        picked = [[] for m in range(share)]
        for e in range(per_group):
            request = my_group * per_group + e
            numer, denom, own = found[a, e]
            result = (numer + own.astype(jnp.bfloat16).astype(jnp.float32) * v_new) / denom
            for m in range(share):
                chosen = jnp.where(row_of == m * B + request, result, 0.0)
                picked[m].append(jnp.sum(chosen, axis=0, keepdims=True))
        for m in range(share):
            at = (a * share + m) * HEAD_DIM
            att[me, :, at : at + HEAD_DIM] = jnp.concatenate(picked[m], axis=0).astype(jnp.bfloat16)
    push(2, att_sem.at[0], att.at[me])
    send_others()

    first_lane = pl.multiple_of(me * R // LANES * LANES, LANES)
    window = RP + LANES
    turn = window - lax.rem(me * R, LANES)
    own_hid = pltpu.roll(hid[:, pl.ds(first_lane, window)], turn, 1)[:, :RP]
    own_gain = pltpu.roll(gain[:, pl.ds(first_lane, window)], turn, 1)[:, :RP]
    wo_load.wait()
    q_width = att.shape[2]
    halves = T // PREFILL_TP
    slots_half = PREFILL_TP // halves
    half_width = slots_half * q_width
    landed(att_sem.at[0], att.at[pl.ds(0, T - 1)])
    pieces = [
        jnp.concatenate(
            [att[g * PREFILL_TP + s].astype(jnp.float32) for g in range(groups)], axis=0
        )
        for s in range(PREFILL_TP)
    ]
    probe = pad_rows(jnp.concatenate(pieces, axis=1).astype(jnp.bfloat16), SUBLANES)
    pair = R // 2
    pair_lane = pair // LANES * LANES
    cut = probe.shape[1] // 2
    sides = [
        dot_t(
            jnp.concatenate([probe[:, k : k + cut], wo[pair:, k : k + cut]], axis=0),
            jnp.concatenate([wo[:pair, k : k + cut], probe[:, k : k + cut]], axis=0),
        )
        for k in (0, cut)
    ]
    flatwise = jnp.concatenate([side[:B, :pair] for side in sides], axis=0)
    flatwise = flatwise[:B] + flatwise[B:]
    upward = [
        jnp.concatenate(
            [
                side[SUBLANES:, pair_lane:],
                jnp.zeros((pair, LANES - (SUBLANES + pair - pair_lane)), jnp.float32),
            ],
            axis=1,
        ).T[pair - pair_lane : pair - pair_lane + B]
        for side in sides
    ]
    mixed = jnp.concatenate([flatwise, upward[0] + upward[1]], axis=1)
    mixed = mixed.astype(jnp.bfloat16).astype(jnp.float32)
    mixed = jnp.concatenate([mixed, jnp.zeros((B, RP - R), jnp.float32)], axis=1)
    shift = dims["seat_shift"]
    mix[me] = pltpu.roll(mixed, my_seat * shift, 1).astype(jnp.bfloat16)
    push(3, mix_sem.at[my_group], mix.at[me], True)
    blend[:B, :] = hid[:, :model] * (1.0 + gain[2:3, :model])
    wgu_load.wait()
    side = ff // 2
    tile = dims["ff_tile"]
    at_lane = tile // LANES * LANES
    blocks = [(s, c) for s in range(side // tile) for c in range(2)]
    half_cols = model // halves
    half_seats = T // halves
    front, upright = {}, {}
    for turn_of in range(halves):
        which = (my_plane // (planes // halves) + turn_of) % halves
        seats = half_seats - 1 if turn_of == 0 else half_seats
        landed(mix_sem.at[which], mix.at[pl.ds(which * half_seats, seats)])
        if turn_of == 0:
            push_pages(dims["page_cut"], T)
        tiles = [None] * (half_cols // LANES)
        for s in range(half_seats):
            block = mix[which * half_seats + s].astype(jnp.float32)
            for i in range(RP // LANES):
                at = s * R // LANES + i
                piece = block[:, i * LANES : (i + 1) * LANES]
                if at < len(tiles):
                    tiles[at] = piece if tiles[at] is None else tiles[at] + piece
        got = jnp.concatenate(tiles, axis=1)
        span_at = pl.ds(pl.multiple_of(which * half_cols, LANES), half_cols)
        mixed_ref[:, span_at] = got
        blend[B:, span_at] = got * ((1.0 + gain[1:2, span_at]) * (1.0 + gain[2:3, span_at]))
        exact = blend[:, span_at]
        high = exact.astype(jnp.bfloat16).astype(jnp.float32)
        probe = jnp.concatenate([high, exact - high], axis=0).astype(jnp.bfloat16)
        if turn_of == halves - 1:
            mixed_all = mixed_ref[...]
            mixed_ms = meansq_of(mixed_all)
            stream = hid[:, :model] + normed_by(mixed_all, mixed_ms, gain[1:2, :model])
            outer = lax.rsqrt(meansq_of(stream) + EPSILON)
            inner = lax.rsqrt(mixed_ms + EPSILON)
            mine = own_hid + normed_by(mixed, mixed_ms, own_gain[1:2, :])
        for s, c in blocks:
            at = s * tile
            pushed = jnp.concatenate([wgu[c, at : at + tile, span_at], probe], axis=0)
            passed = jnp.concatenate(
                [probe, wgu[c, side + at : side + at + tile, span_at]], axis=0
            )
            both = dot_t(passed, pushed)
            part = both[: 2 * B, :tile] + both[2 * B : 4 * B, :tile]
            front[s, c] = part if turn_of == 0 else front[s, c] + part
            rest = both[4 * B :, at_lane:]
            wide = rest.shape[1]
            if turn_of < halves - 1:
                stack[s, c, :, :wide] = rest
            else:
                rest = jnp.concatenate([rest, jnp.zeros((tile, LANES - wide), jnp.float32)], axis=1)
                first = tile - at_lane
                turned = [(piece.T)[first : first + 4 * B] for piece in (rest, stack[s, c])]
                turned = turned[0] + turned[1]
                upright[s, c] = turned[: 2 * B] + turned[2 * B :]

    def settle(parts):
        return outer * (parts[:B] + inner * parts[B:])

    steps = range(side // tile)
    active = []
    for table_of in (front, upright):
        for s in steps:
            gate, up = settle(table_of[s, 0]), settle(table_of[s, 1])
            active.append(jax.nn.gelu(gate, approximate=True) * up)
    active = jnp.concatenate(active, axis=1).astype(jnp.bfloat16)
    wd_load.wait()
    owned = model // owner_count
    span = arrive.shape[2]
    is_owner = (me >= first_owner) & (me < first_owner + owner_count)
    side_owners = owner_count // halves
    for turn_of in range(halves):
        which = (halves - 1 - my_plane // (planes // halves) + turn_of) % halves
        half_at = pl.multiple_of(which * half_cols, LANES)
        wide = -(-half_cols // (4 * LANES)) * 4 * LANES
        done_cols = wide if turn_of == 0 else model - wide
        done_at = pl.multiple_of(which * (model - done_cols), LANES)
        part = jnp.dot(active, wd[:, pl.ds(done_at, done_cols)], preferred_element_type=jnp.float32)
        branch[:, pl.ds(done_at, done_cols)] = part.astype(jnp.bfloat16)
        for i in range(side_owners):
            peer = first_owner + which * side_owners + i

            @pl.when(me != peer)
            def _():
                begin = pl.multiple_of(half_at + i * owned // LANES * LANES, LANES)
                remote(branch.at[:, pl.ds(begin, span)], arrive.at[me], 4, tail_sem.at[0], peer).start()

    @pl.when(is_owner)
    def _():
        o = me - first_owner
        odd = o % 2
        base = pl.multiple_of(o * owned // LANES * LANES, LANES)
        total = branch[:, pl.ds(base, span)].astype(jnp.float32)
        landed(tail_sem.at[0], arrive.at[pl.ds(0, T - 1)])
        for s in range(T):
            piece = arrive[s].astype(jnp.float32)
            total = total + jnp.where(me == s, 0.0, piece)
        offset = odd * (LANES // 2)
        lane_of = lax.broadcasted_iota(jnp.int32, (B, span), 1)
        inside = (lane_of >= offset) & (lane_of < offset + owned)
        kept = jnp.where(inside, total, 0.0)
        each = jnp.sum(kept * kept, axis=-1, keepdims=True)
        spot = lax.broadcasted_iota(jnp.int32, (B, LANES), 1) == lax.broadcasted_iota(
            jnp.int32, (B, LANES), 0
        )
        squares[o] = jnp.sum(jnp.where(spot, each, 0.0), axis=0, keepdims=True)
        push(6, tail_sem.at[2], squares.at[o])
        ready = []
        for i in range(2):
            begin = i * R // LANES * LANES
            left = RP - (i * R - begin) - offset
            ready.append(pltpu.roll(kept[:, begin : begin + RP], lax.rem(left, RP), 1))
            sums[i] = ready[i]
        for i in range(2):
            peer = o * 2 + i

            @pl.when(peer != me)
            def _():
                remote(sums.at[i], sums.at[2], 5, tail_sem.at[1], peer).start()

            @pl.when(peer == me)
            def _():
                sums[2] = ready[i]

    dec_part(dec, me)[...] = page_stage[me]
    landed(tail_sem.at[3], page_stage.at[pl.ds(0, T - 1)])
    for owner in range(q_devs, q_devs + 2 * k_devs):
        @pl.when((owner != k_from) & (owner != v_from))
        def _():
            take_proj(jnp.int32(owner))

    token = lax.broadcasted_iota(jnp.int32, (page_width, cols), 0) + me * page_width
    for c in range(2):
        for i in range(k_devs):
            fresh = proj[q_devs + c * k_devs + i].astype(jnp.float32)
            for r in range(B):
                old = dec[c, r, :, i * cols : (i + 1) * cols].astype(jnp.float32)
                row = jnp.broadcast_to(fresh[r : r + 1, :], old.shape)
                new = jnp.where(token == len_ref[r], row, old)
                dec_done[c, r, :, i * cols : (i + 1) * cols] = new.astype(jnp.bfloat16)

    for send, ref in ((2, att), (3, mix)):
        sent(send, ref.at[pl.ds(0, T - 1)])
    sent(1, page_stage.at[pl.ds(0, T - 1)])

    @pl.when(me < q_devs)
    def _():
        sent(0, proj.at[0])

    @pl.when(me >= q_devs)
    def _():
        sent(0, proj.at[pl.ds(0, T - 1)])

    @pl.when(is_owner)
    def _():
        sent(4, arrive.at[pl.ds(0, owner_count - 1)])
        landed(tail_sem.at[2], squares.at[pl.ds(0, owner_count - 1)])

    @pl.when(jnp.logical_not(is_owner))
    def _():
        sent(4, arrive.at[pl.ds(0, owner_count)])
        landed(tail_sem.at[2], squares.at[pl.ds(0, owner_count)])

    @pl.when(first_owner + me // 2 != me)
    def _():
        landed(tail_sem.at[1], sums.at[2])

    sumsq = squares[0]
    for s in range(1, owner_count):
        sumsq = sumsq + squares[s]
    spot = lax.broadcasted_iota(jnp.int32, (B, LANES), 1) == lax.broadcasted_iota(
        jnp.int32, (B, LANES), 0
    )
    branch_ms = jnp.sum(
        jnp.where(spot, jnp.broadcast_to(sumsq, (B, LANES)), 0.0), axis=-1, keepdims=True
    ) * (1.0 / model)
    result = mine + normed_by(sums[2], branch_ms, own_gain[3:4, :])
    out_ref[...] = result[:, :R]

    @pl.when(is_owner)
    def _():
        o = me - first_owner
        sent(6, arrive_like(squares, T - 1, owner_count))

        @pl.when(o * 2 == me)
        def _():
            sent(5, sums.at[0])

        @pl.when(o * 2 + 1 == me)
        def _():
            sent(5, sums.at[0])

        @pl.when((o * 2 != me) & (o * 2 + 1 != me))
        def _():
            sent(5, sums.at[pl.ds(0, 2)])


def arrive_like(squares, count, limit):
    return squares.at[pl.ds(0, count)]


def finish_kernel(out_ref, dec_ref, out_hbm, dec_hbm, sem):
    first = pltpu.make_async_copy(dec_ref, dec_hbm, sem.at[0])
    second = pltpu.make_async_copy(out_ref, out_hbm, sem.at[1])
    first.start()
    second.start()
    first.wait()
    second.wait()


def fits_kernel(shapes, devices):
    batch_rows, model = shapes["hidden"]
    cols, rows, ff = shapes["qkv"], shapes["out"], shapes["ff"]
    groups = devices // PREFILL_TP
    weight_bytes = 2 * (cols * model + rows * HEADS * HEAD_DIM + 3 * ff * model)
    return (
        devices == 2 * PREFILL_TP
        and cols == HEADS // PREFILL_TP * HEAD_DIM
        and (KV_HEADS * HEAD_DIM) % cols == 0
        and (HEADS * HEAD_DIM) % cols == 0
        and batch_rows % groups == 0
        and model % (LANES * 2) == 0
        and ff % (6 * SUBLANES) == 0
        and rows * devices == model
        and rows * 4 % LANES == 0
        and rows % (2 * SUBLANES) == 0
        and weight_bytes < VMEM_LIMIT * 3 // 4
        and batch_rows == 4
    )


SUBLANES = 16


def fused_device(
    hidden_in,
    prefill_cache,
    lengths,
    page_table,
    qkv_weight,
    out_weight,
    gate_up_weight,
    down_weight,
    norm_gains,
):
    T = lax.axis_size("tp")
    B, model = hidden_in.shape
    groups = T // PREFILL_TP
    per_group = B // groups
    local_heads = KV_HEADS // PREFILL_TP
    share = HEADS // KV_HEADS
    pages, page_width, width = prefill_cache.shape[4:]
    S = pages * page_width
    cols = qkv_weight.shape[1]
    R = out_weight.shape[1]
    RP = -(-R // LANES) * LANES
    ff = down_weight.shape[1]
    k_cols = KV_HEADS * HEAD_DIM
    planes = 4
    plane_size = T // planes
    owner_count = T // 2
    depth = model // 256
    marks = list(range(0, depth, 2)) + [depth]
    dims = dict(
        T=T, B=B, R=R, RP=RP, S=S, share=share, local_heads=local_heads,
        per_group=per_group, groups=groups, planes=planes, plane_size=plane_size,
        first_owner=plane_size, owner_count=owner_count, seat_shift=R % LANES,
        cuts=[(lo * 256, hi * 256) for lo, hi in zip(marks, marks[1:])],
        ff_tile=ff // 6, page_cut=6,
    )
    q_width = local_heads * share * HEAD_DIM
    span = -(-(model // owner_count) // LANES) * LANES
    bf16, f32 = jnp.bfloat16, jnp.float32
    vmem = pl.BlockSpec(memory_space=pltpu.VMEM)
    anyw = pl.BlockSpec(memory_space=pl.ANY)
    out, dec = pl.pallas_call(
        functools.partial(fused_kernel, dims),
        out_shape=(
            pltpu.VMEM((B, R), f32),
            pltpu.VMEM((2, B, page_width, k_cols), bf16),
        ),
        in_specs=[anyw] * 9,
        out_specs=(vmem, vmem),
        scratch_shapes=[
            pltpu.SMEM((B,), jnp.int32),
            pltpu.VMEM((B, model + RP), f32),
            pltpu.VMEM((norm_gains.shape[1], model + RP), f32),
            pltpu.VMEM((B, T), jnp.int32),
            pltpu.VMEM((2, per_group, S, width), bf16),
            pltpu.VMEM((cols, model), bf16),
            pltpu.VMEM((R, HEADS * HEAD_DIM), bf16),
            pltpu.VMEM((2, ff, model), bf16),
            pltpu.VMEM((ff, model), bf16),
            pltpu.VMEM((T, B, cols), bf16),
            pltpu.VMEM((T, per_group, q_width), bf16),
            pltpu.VMEM((B, HEADS * HEAD_DIM), bf16),
            pltpu.VMEM((T, B, RP), bf16),
            pltpu.VMEM((B, model), bf16),
            pltpu.VMEM((T, B, span), bf16),
            pltpu.VMEM((3, B, RP), f32),
            pltpu.VMEM((T, 1, LANES), f32),
            pltpu.VMEM((3, 2, ff // 6, LANES), f32),
            pltpu.VMEM((B, model), f32),
            pltpu.VMEM((2 * B, model), f32),
            pltpu.VMEM((T, 2, per_group, page_width, width), bf16),
            pltpu.VMEM((2, B, page_width, k_cols), bf16),
            pltpu.SemaphoreType.DMA((8 + len(dims["cuts"]),)),
            pltpu.SemaphoreType.DMA((7,)),
            pltpu.SemaphoreType.DMA((9,)),
            pltpu.SemaphoreType.DMA((1,)),
            pltpu.SemaphoreType.DMA((2,)),
            pltpu.SemaphoreType.DMA((4,)),
        ],
        compiler_params=pltpu.CompilerParams(
            collective_id=0, has_side_effects=True, vmem_limit_bytes=VMEM_LIMIT
        ),
    )(
        lengths,
        page_table,
        hidden_in,
        norm_gains[0],
        prefill_cache.reshape(2, per_group, S, width),
        qkv_weight[0],
        out_weight[0],
        gate_up_weight[0],
        down_weight[0],
    )
    out, dec = pl.pallas_call(
        finish_kernel,
        out_shape=(
            jax.ShapeDtypeStruct((B, R), f32),
            jax.ShapeDtypeStruct((2, B, page_width, k_cols), bf16),
        ),
        in_specs=[vmem, vmem],
        out_specs=(anyw, anyw),
        scratch_shapes=[pltpu.SemaphoreType.DMA((2,))],
    )(
        pltpu.with_memory_space_constraint(out, pltpu.VMEM),
        pltpu.with_memory_space_constraint(dec, pltpu.VMEM),
    )
    return out, dec.reshape(1, 1, 2, B, page_width, k_cols)


def step(*args):
    shapes = {
        "hidden": args[0].shape,
        "qkv": args[4].shape[1],
        "out": args[5].shape[1],
        "ff": args[7].shape[1],
    }
    chosen = fused_device if fits_kernel(shapes, lax.axis_size("tp")) else on_device
    return chosen(*args)


def solution(mesh):
    placed = (
        P("grp", None),
        P("tp", None, None, "grp", None, None, None),
        P("grp"),
        P("grp", None),
        P(None, "tp", None),
        P(None, "tp", None),
        P(None, None, "tp", None),
        P(None, "tp", None),
        P(),
    )
    return jax.shard_map(
        step,
        mesh=mesh,
        in_specs=placed,
        out_specs=(P("grp", "tp"), P("tp", None, None, "grp", None, None)),
        check_vma=False,
    )
```
